32 devices in a mesh: data: 4 (over x, y), tp: 8 (over z, core).
Axes of the slice: x: 2, y: 2, z: 4, core: 2. Of those that a mesh axis runs over, the one named last changes fastest.
Arguments:
- X: bfloat16 [16384, 1280], P(('data', 'tp')), parts along dimension 0
- gamma: float32 [1280], replicated
- W1: bfloat16 [1280, 5120], P(None, 'tp')
- W2: bfloat16 [5120, 1280], P('tp')
- dY: bfloat16 [16384, 1280], P(('data', 'tp')), parts along dimension 0
Outputs:
- output 1: bfloat16 [16384, 1280], P(('data', 'tp')), parts along dimension 0
- output 2: bfloat16 [16384, 1280], P(('data', 'tp')), parts along dimension 0
- output 3: float32 [5120, 5120], P('data', 'tp'), parts along dimension 0
- output 4: float32 [20480, 1280], P(('data', 'tp')), parts along dimension 0
- output 5: float32 [5120], P('data'), parts along dimension 0
There are 4 independent parts. The reference program is written for one: setup_inputs(seed, part) draws one part's arguments, and reference() takes and returns one part's arrays. A program takes and returns all parts, laid end to end along the dimension named above; an argument that names none is the same for every part.
All inputs are finite; a program needn't handle non-finite values.
Results may differ from the reference program's by a relative error of at most 0.001.
Values are sent between devices in bfloat16 or wider.
A program may use at most 1 GiB of HBM per device.

```python
import jax
import jax.numpy as jnp
from jax import lax

S = 4096
D = 1280
F = 5120
EPS = 1e-6


def setup_inputs(seed: int = 0, part: int = 0) -> dict:
    key = jax.random.key(seed)
    kg, k1, k2, kbase = jax.random.split(key, 4)
    kx, ky = jax.random.split(jax.random.fold_in(kbase, part))
    X = jax.random.normal(kx, (S, D), jnp.float32).astype(jnp.bfloat16)
    gamma = 1.0 + 0.2 * jax.random.normal(kg, (D,), jnp.float32)
    W1 = (jax.random.normal(k1, (D, F), jnp.float32) * D ** -0.5).astype(jnp.bfloat16)
    W2 = (jax.random.normal(k2, (F, D), jnp.float32) * (1.5 * F ** -0.5)).astype(jnp.bfloat16)
    dY = jax.random.normal(ky, (S, D), jnp.float32).astype(jnp.bfloat16)
    return {"X": X, "gamma": gamma, "W1": W1, "W2": W2, "dY": dY}


def _gelu(a):
    return jax.nn.gelu(a, approximate=True)


def reference(X, gamma, W1, W2, dY):
    x = X.astype(jnp.float32)
    mu = jnp.mean(x, axis=-1, keepdims=True)
    xc = x - mu
    var = jnp.mean(xc * xc, axis=-1, keepdims=True)
    rstd = lax.rsqrt(var + EPS)
    xhatv = xc * rstd
    Xn = (xhatv * gamma).astype(jnp.bfloat16)
    A = jnp.dot(Xn, W1, preferred_element_type=jnp.float32)
    H = _gelu(A).astype(jnp.bfloat16)
    Y = (x + jnp.dot(H, W2, preferred_element_type=jnp.float32)).astype(jnp.bfloat16)
    dW2 = jnp.dot(H.T, dY, preferred_element_type=jnp.float32)
    dH = jnp.dot(dY, W2.T, preferred_element_type=jnp.float32)
    dA = jax.vjp(_gelu, A)[1](dH)[0].astype(jnp.bfloat16)
    dW1 = jnp.dot(Xn.T, dA, preferred_element_type=jnp.float32)
    dXn = jnp.dot(dA, W1.T, preferred_element_type=jnp.float32)
    dgamma = jnp.sum(dXn * xhatv, axis=0)
    dxhat = dXn * gamma
    dx = rstd * (dxhat - jnp.mean(dxhat, axis=-1, keepdims=True) - xhatv * jnp.mean(dxhat * xhatv, axis=-1, keepdims=True))
    dX = (dY.astype(jnp.float32) + dx).astype(jnp.bfloat16)
    return (Y, dX, dW1, dW2, dgamma)
```

```python
import functools

import jax
import jax.numpy as jnp
from jax import lax
from jax.experimental import pallas as pl
from jax.experimental.pallas import tpu as pltpu
from jax.sharding import PartitionSpec as P

EPS = 1e-6
D = 1280
TOK = 512
FF = 640
NH = 2
TH = TOK // NH
NB = 256
RT = 64
K0 = 0.7978845608028654
K1 = 0.044715
MESH = pl.DeviceIdType.MESH


def _nt(a, b):
    return lax.dot_general(a, b, (((1,), (1,)), ((), ())), preferred_element_type=jnp.float32)


def _nn(a, b):
    return lax.dot_general(a, b, (((1,), (0,)), ((), ())), preferred_element_type=jnp.float32)


def _ln(x):
    mu = jnp.mean(x, axis=-1, keepdims=True)
    xc = x - mu
    var = jnp.mean(xc * xc, axis=-1, keepdims=True)
    rstd = lax.rsqrt(var + EPS)
    return xc * rstd, rstd


def _gelu_pair(a, g):
    a2 = a * a
    t = jnp.tanh(a * (K0 + (K0 * K1) * a2))
    cdf = 0.5 + 0.5 * t
    h = a * cdf
    dg = cdf + h * (1.0 - t) * (K0 + (3.0 * K0 * K1) * a2)
    return h.astype(jnp.bfloat16), (dg * g).astype(jnp.bfloat16)


def _kernel(x_h, g_ref, w1_h, w2_h, dy_h, y_h, dx_h, dw1_h, dw2_h, dg_ref,
            T, W, yacc, wacc, xb, ob, dgb,
            lsem, osem, tsend, trecv, wsend, wrecv, dgs, dgr):
    d = lax.axis_index("data")
    t = lax.axis_index("tp")
    z = t // 2
    c = t - 2 * z
    o = 1 - c
    partner = (d, 2 * z + o)
    up = (d, 2 * z + 2 + c)
    down = (d, 2 * z - 2 + c)
    dxn = lax.rem(d + 2, 4)
    dyn = d + 1 - 2 * lax.rem(d, 2)
    ddg = 3 - d
    side = ((dxn, 3), (dyn, 4), (ddg, 5))

    def tslot(src, lane, h):
        return T.at[src, :, pl.ds(pl.multiple_of(lane * TOK + h * TH, TH), TH), :]

    def tcopy(src, lane, h, path, dev):
        s = tslot(src, lane, h)
        return pltpu.make_async_remote_copy(
            src_ref=s, dst_ref=s, send_sem=tsend.at[src, h, path],
            recv_sem=trecv.at[src, lane, h], device_id=dev, device_id_type=MESH)

    def wcopy(src, lane, q, path, dev):
        s = W.at[src, :, pl.ds(pl.multiple_of(lane * FF + q * (FF // 4), 32), FF // 4), :]
        return pltpu.make_async_remote_copy(
            src_ref=s, dst_ref=s, send_sem=wsend.at[src, q, path],
            recv_sem=wrecv.at[src, lane, q], device_id=dev, device_id_type=MESH)

    def wown(lane):
        s = W.at[z, :, pl.ds(pl.multiple_of(lane * FF, FF), FF), :]
        return pltpu.make_async_remote_copy(
            src_ref=s, dst_ref=s, send_sem=wsend.at[z, 0, 2],
            recv_sem=wrecv.at[z, lane, 0], device_id=partner, device_id_type=MESH)

    frow = pl.ds(pl.multiple_of(c * FF, FF), FF)
    trow = pl.ds(pl.multiple_of(c * TOK, TOK), TOK)
    l1 = pltpu.make_async_copy(w1_h, W.at[z, 0, frow, :], lsem.at[0])
    l2 = pltpu.make_async_copy(w2_h, W.at[z, 1, frow, :], lsem.at[1])
    l3 = pltpu.make_async_copy(x_h, xb, lsem.at[2])
    l4 = pltpu.make_async_copy(dy_h, T.at[z, 1, trow, :], lsem.at[3])
    l1.start(); l2.start(); l3.start(); l4.start()
    l1.wait(); l2.wait()

    @pl.when(z < 3)
    def _():
        wcopy(z, c, d, 0, up).start()

    @pl.when(z > 0)
    def _():
        wcopy(z, c, d, 1, down).start()

    wown(c).start()
    l3.wait()

    @pl.loop(0, TOK // RT)
    def _(i):
        r = pl.ds(pl.multiple_of(i * RT, RT), RT)
        x = xb[r, :].astype(jnp.float32)
        xh, _ = _ln(x)
        T[z, 0, pl.ds(pl.multiple_of(c * TOK + i * RT, RT), RT), :] = (xh * g_ref[...]).astype(jnp.bfloat16)
        yacc[1, r, :] = x
        yacc[0, r, :] = jnp.zeros((RT, D), jnp.float32)

    l4.wait()

    @pl.loop(0, FF // RT)
    def _(i):
        r = pl.ds(pl.multiple_of(i * RT, RT), RT)
        wacc[0, r, :] = jnp.zeros((RT, D), jnp.float32)
        wacc[1, r, :] = jnp.zeros((RT, D), jnp.float32)

    def tup():
        for h in range(NH):
            tcopy(z, c, h, 0, up).start()

    def tdown():
        for h in range(NH):
            tcopy(z, c, h, 1, down).start()

    pl.when(z == 0)(tup)
    pl.when(z == 3)(tdown)
    for h in range(NH):
        tcopy(z, c, h, 2, partner).start()

    for s in range(1, 4):
        for sgn in (-1, 1):
            src = z + sgn * s

            @pl.when((src >= 0) & (src <= 3))
            def _():
                wcopy(src, c, d, 0, up).wait_recv()

                @pl.when((z + (-sgn) >= 0) & (z + (-sgn) <= 3))
                def _():
                    wcopy(src, c, d, 0, (d, 2 * (z - sgn) + c)).start()

                for dd, path in side:
                    wcopy(src, c, d, path, (dd, t)).start()
                wcopy(src, c, d, 2, partner).start()

        if s < 3:
            pl.when(z == s)(tup)
            pl.when(z == 3 - s)(tdown)

    def block(L, li, lrow, m, R, ri, r0, nb, acc):
        rr = pl.ds(pl.multiple_of(r0, 128), nb)
        lr = pl.ds(pl.multiple_of(lrow, 128), m)
        a = _nt(L[li, 0, lr, :], R[ri, 0, rr, :])
        g = _nt(L[li, 1, lr, :], R[ri, 1, rr, :])
        h, da = _gelu_pair(a, g)
        acc[1, :, :] += _nn(h, R[ri, 1, rr, :])
        acc[0, :, :] += _nn(da, R[ri, 0, rr, :])

    elast = jnp.where(z == 0, 6, jnp.where(z == 3, 5, jnp.where(z == 1, 4, 3)))

    @pl.loop(0, 7)
    def _(e):
        s = (e + 1) // 2
        sgn = 1 - 2 * (e - 2 * (e // 2))
        src = z + sgn * s
        nxt = z - sgn

        @pl.when((src >= 0) & (src <= 3))
        def _():
            @pl.when(e == 0)
            def _():
                wown(o).wait_recv()

            @pl.when(e > 0)
            def _():
                for dd, _p in side:
                    wcopy(src, c, dd, 2, partner).wait_recv()
                    wcopy(src, c, dd, 2, partner).start()
                for q in range(4):
                    wcopy(src, o, q, 2, partner).wait_recv()

            @pl.loop(0, 2 * FF // NB)
            def _(i):
                block(T, z, c * TOK, TOK, W, src, i * NB, NB, yacc)

            @pl.when(e == elast)
            def _():
                dgb[t] = jnp.zeros((8, D), jnp.float32)

                @pl.loop(0, TOK // RT)
                def _(i):
                    r = pl.ds(pl.multiple_of(i * RT, RT), RT)
                    x = xb[r, :].astype(jnp.float32)
                    xh, rstd = _ln(x)
                    dxn_ = yacc[0, r, :]
                    p = dxn_ * xh
                    dgb[t] += jnp.sum(p.reshape(RT // 8, 8, D), axis=0)
                    dxh = dxn_ * g_ref[...]
                    m1 = jnp.mean(dxh, axis=-1, keepdims=True)
                    m2 = jnp.mean(dxh * xh, axis=-1, keepdims=True)
                    dyv = T[z, 1, pl.ds(pl.multiple_of(c * TOK + i * RT, RT), RT), :].astype(jnp.float32)
                    ob[r, :] = (dyv + rstd * (dxh - m1 - xh * m2)).astype(jnp.bfloat16)
                    xb[r, :] = yacc[1, r, :].astype(jnp.bfloat16)

                pltpu.make_async_copy(xb, y_h, osem.at[0]).start()
                pltpu.make_async_copy(ob, dx_h, osem.at[1]).start()
                for k in range(1, 8):
                    pltpu.make_async_remote_copy(
                        src_ref=dgb.at[t], dst_ref=dgb.at[t], send_sem=dgs.at[k],
                        recv_sem=dgr.at[k], device_id=(d, lax.rem(t + k, 8)),
                        device_id_type=MESH).start()

            for h in range(NH):
                @pl.when(e > 0)
                def _():
                    tcopy(src, c, h, 0, up).wait_recv()

                    @pl.when((nxt >= 0) & (nxt <= 3))
                    def _():
                        tcopy(src, c, h, 0, (d, 2 * nxt + c)).start()

                    tcopy(src, c, h, 2, partner).start()

            @pl.loop(0, NH)
            def _(h):
                @pl.loop(0, 2)
                def _(j):
                    lane = c + j * (1 - 2 * c)

                    @pl.when(j == 1)
                    def _():
                        tcopy(src, o, h, 2, partner).wait_recv()

                    block(W, z, c * FF, FF, T, src, lane * TOK + h * TH, TH, wacc)

    ow1 = pltpu.make_async_copy(wacc.at[0], dw1_h, osem.at[2])
    ow2 = pltpu.make_async_copy(wacc.at[1], dw2_h, osem.at[3])
    ow1.start()
    ow2.start()

    for k in range(1, 8):
        pltpu.make_async_remote_copy(
            src_ref=dgb.at[t], dst_ref=dgb.at[t], send_sem=dgs.at[k],
            recv_sem=dgr.at[k], device_id=partner, device_id_type=MESH).wait_recv()
    tot = jnp.sum(dgb[...], axis=0)
    dg_ref[...] = jnp.sum(tot, axis=0, keepdims=True)

    for k in range(1, 8):
        pltpu.make_async_remote_copy(
            src_ref=dgb.at[t], dst_ref=dgb.at[t], send_sem=dgs.at[k],
            recv_sem=dgr.at[k], device_id=partner, device_id_type=MESH).wait_send()
    wown(c).wait_send()

    @pl.when(z < 3)
    def _():
        wcopy(z, c, d, 0, up).wait_send()
        for h in range(NH):
            tcopy(z, c, h, 0, up).wait_send()

    @pl.when(z > 0)
    def _():
        wcopy(z, c, d, 1, down).wait_send()
        for h in range(NH):
            tcopy(z, c, h, 1, down).wait_send()

    for h in range(NH):
        tcopy(z, c, h, 2, partner).wait_send()

    @pl.loop(1, 7)
    def _(e):
        s = (e + 1) // 2
        sgn = 1 - 2 * (e - 2 * (e // 2))
        src = z + sgn * s
        nxt = z - sgn

        @pl.when((src >= 0) & (src <= 3))
        def _():
            @pl.when((nxt >= 0) & (nxt <= 3))
            def _():
                wcopy(src, c, d, 0, up).wait_send()
                for h in range(NH):
                    tcopy(src, c, h, 0, up).wait_send()

            for dd, path in side:
                wcopy(src, c, d, path, partner).wait_send()
                wcopy(src, c, dd, 2, partner).wait_send()
            wcopy(src, c, d, 2, partner).wait_send()
            for h in range(NH):
                tcopy(src, c, h, 2, partner).wait_send()

    pltpu.make_async_copy(xb, y_h, osem.at[0]).wait()
    pltpu.make_async_copy(ob, dx_h, osem.at[1]).wait()
    ow1.wait()
    ow2.wait()


def solution(mesh):
    rows = P(("data", "tp"), None)
    bf, f32 = jnp.bfloat16, jnp.float32

    def body(X, gamma, W1, W2, dY):
        hbm = pl.BlockSpec(memory_space=pl.ANY)
        vm = pl.BlockSpec(memory_space=pltpu.VMEM)
        Y, dX, dW1t, dW2, dg = pl.pallas_call(
            _kernel,
            name="mlp_block",
            out_shape=(jax.ShapeDtypeStruct((TOK, D), bf), jax.ShapeDtypeStruct((TOK, D), bf),
                       jax.ShapeDtypeStruct((FF, D), f32), jax.ShapeDtypeStruct((FF, D), f32),
                       jax.ShapeDtypeStruct((1, D), f32)),
            in_specs=[hbm, vm, hbm, hbm, hbm],
            out_specs=[hbm, hbm, hbm, hbm, vm],
            scratch_shapes=[
                pltpu.VMEM((4, 2, 2 * TOK, D), bf),
                pltpu.VMEM((4, 2, 2 * FF, D), bf),
                pltpu.VMEM((2, TOK, D), f32),
                pltpu.VMEM((2, FF, D), f32),
                pltpu.VMEM((TOK, D), bf),
                pltpu.VMEM((TOK, D), bf),
                pltpu.VMEM((8, 8, D), f32),
                pltpu.SemaphoreType.DMA((4,)),
                pltpu.SemaphoreType.DMA((4,)),
                pltpu.SemaphoreType.DMA((4, NH, 3)),
                pltpu.SemaphoreType.DMA((4, 2, NH)),
                pltpu.SemaphoreType.DMA((4, 4, 6)),
                pltpu.SemaphoreType.DMA((4, 2, 4)),
                pltpu.SemaphoreType.DMA((8,)),
                pltpu.SemaphoreType.DMA((8,)),
            ],
            compiler_params=pltpu.CompilerParams(has_side_effects=True, vmem_limit_bytes=67043328),
        )(X, gamma.reshape(1, D), W1.T, W2, dY)
        return Y, dX, dW1t.T, dW2, dg.reshape(D)

    return jax.shard_map(body, mesh=mesh,
                         in_specs=(rows, P(None), P(None, "tp"), P("tp", None), rows),
                         out_specs=(rows, rows, P("data", "tp"), rows, P("data")),
                         check_vma=False)
```

```python
import functools

import jax
import jax.numpy as jnp
from jax import lax
from jax.experimental import pallas as pl
from jax.experimental.pallas import tpu as pltpu
from jax.sharding import PartitionSpec as P

EPS = 1e-6
D = 1280
TOK = 512
FF = 640
NH = 4
TH = TOK // NH
NB = 256
RT = 64
VM1 = 60 * 2**20
VM2 = 60 * 2**20
K0 = 0.7978845608028654
K1 = 0.044715
MESH = pl.DeviceIdType.MESH


def _nt(a, b):
    return lax.dot_general(a, b, (((1,), (1,)), ((), ())), preferred_element_type=jnp.float32)


def _nn(a, b):
    return lax.dot_general(a, b, (((1,), (0,)), ((), ())), preferred_element_type=jnp.float32)


def _tn(a, b):
    return lax.dot_general(a, b, (((0,), (0,)), ((), ())), preferred_element_type=jnp.float32)


def _ln(x):
    mu = jnp.mean(x, axis=-1, keepdims=True)
    xc = x - mu
    var = jnp.mean(xc * xc, axis=-1, keepdims=True)
    rstd = lax.rsqrt(var + EPS)
    return xc * rstd, rstd


def _gelu_pair(a, g):
    a2 = a * a
    t = jnp.tanh(a * (K0 + (K0 * K1) * a2))
    cdf = 0.5 + 0.5 * t
    h = a * cdf
    dg = cdf + h * (1.0 - t) * (K0 + (3.0 * K0 * K1) * a2)
    return h.astype(jnp.bfloat16), (dg * g).astype(jnp.bfloat16)


def _kernel(x_h, g_ref, w1_h, w2_h, dy_h, y_h, dx_h, dw1_h, dw2_h, tl_h, W, dg_ref,
            T, wo, wb, yacc, wacc, wt, xb, ob, dgb,
            w1n, lsem, osem, bsem, tsend, trecv, wsend, wrecv, dgs, dgr):
    d = lax.axis_index("data")
    t = lax.axis_index("tp")
    z = t // 2
    c = t - 2 * z
    o = 1 - c
    partner = (d, 2 * z + o)
    up = (d, 2 * z + 2 + c)
    down = (d, 2 * z - 2 + c)
    dxn = lax.rem(d + 2, 4)
    dyn = d + 1 - 2 * lax.rem(d, 2)
    ddg = 3 - d
    side = ((dxn, 3), (dyn, 4), (ddg, 5))

    def tslot(src, lane, h):
        return T.at[src, :, h, lane]

    def tcopy(src, lane, h, path, dev):
        s = tslot(src, lane, h)
        return pltpu.make_async_remote_copy(
            src_ref=s, dst_ref=s, send_sem=tsend.at[src, h, path],
            recv_sem=trecv.at[src, lane, h], device_id=dev, device_id_type=MESH)

    def wcopy(src, lane, q, path, dev):
        s = W.at[src, :, pl.ds(pl.multiple_of(lane * FF + q * (FF // 4), 32), FF // 4), :]
        return pltpu.make_async_remote_copy(
            src_ref=s, dst_ref=s, send_sem=wsend.at[src, q, path],
            recv_sem=wrecv.at[src, lane, q], device_id=dev, device_id_type=MESH)

    def wown(lane):
        return pltpu.make_async_remote_copy(
            src_ref=wo, dst_ref=W.at[z, :, pl.ds(pl.multiple_of(lane * FF, FF), FF), :], send_sem=wsend.at[z, 0, 2],
            recv_sem=wrecv.at[z, lane, 0], device_id=partner, device_id_type=MESH)

    frow = pl.ds(pl.multiple_of(c * FF, FF), FF)
    l1 = pltpu.make_async_copy(w1_h, w1n, lsem.at[0])
    l2 = pltpu.make_async_copy(w2_h, wo.at[1], lsem.at[1])
    l3 = pltpu.make_async_copy(x_h, xb, lsem.at[2])
    l1.start()
    l2.start()
    l3.start()
    l4 = [pltpu.make_async_copy(dy_h.at[pl.ds(h * TH, TH), :], T.at[z, 1, h, c], lsem.at[3 + h])
          for h in range(NH)]
    for cp in l4:
        cp.start()
    barrier = pltpu.get_barrier_semaphore()
    for k in range(1, 8):
        pl.semaphore_signal(barrier, inc=1, device_id=(d, lax.rem(t + k, 8)), device_id_type=MESH)
    for dd, _p in side:
        pl.semaphore_signal(barrier, inc=1, device_id=(dd, t), device_id_type=MESH)
    pl.semaphore_wait(barrier, 10)

    def whalf(mat, path, dev):
        q = pl.ds(pl.multiple_of(d * (FF // 4), 32), FF // 4)
        return pltpu.make_async_remote_copy(
            src_ref=w2_h.at[q, :] if mat else wo.at[0, q, :],
            dst_ref=W.at[z, mat, pl.ds(pl.multiple_of(c * FF + d * (FF // 4), 32), FF // 4), :], send_sem=wsend.at[z, d, path],
            recv_sem=wrecv.at[z, c, d], device_id=dev, device_id_type=MESH)

    @pl.when(z < 3)
    def _():
        whalf(1, 0, up).start()

    @pl.when(z > 0)
    def _():
        whalf(1, 1, down).start()

    l1.wait()

    for i in range(FF // 128):
        wo[0, i * 128:(i + 1) * 128, :] = w1n[:, i * 128:(i + 1) * 128].T

    l2.wait()
    l3.wait()

    @pl.loop(0, TOK // RT)
    def _(i):
        r = pl.ds(pl.multiple_of(i * RT, RT), RT)
        x = xb[r, :].astype(jnp.float32)
        xh, _ = _ln(x)
        h = i // (TH // RT)
        rr = pl.ds(pl.multiple_of((i - h * (TH // RT)) * RT, RT), RT)
        T[z, 0, h, c, rr, :] = (xh * g_ref[...].reshape(1, D)).astype(jnp.bfloat16)
        yacc[1, r, :] = x
        yacc[0, r, :] = jnp.zeros((RT, D), jnp.float32)

    @pl.when(z < 3)
    def _():
        whalf(0, 0, up).start()

    @pl.when(z > 0)
    def _():
        whalf(0, 1, down).start()

    wown(c).start()
    lo = pltpu.make_async_copy(wo, W.at[z, :, frow, :], lsem.at[3 + NH])
    lo.start()

    @pl.loop(0, FF // RT)
    def _(i):
        r = pl.ds(pl.multiple_of(i * RT, RT), RT)
        wacc[0, r, :] = jnp.zeros((RT, D), jnp.float32)
        wacc[1, r, :] = jnp.zeros((RT, D), jnp.float32)

    for cp in l4:
        cp.wait()

    def town(h0, h1):
        @pl.when(z < 3)
        def _():
            for h in range(h0, h1):
                tcopy(z, c, h, 0, up).start()

        @pl.when(z > 0)
        def _():
            for h in range(h0, h1):
                tcopy(z, c, h, 1, down).start()

    town(0, NH // 2)
    for h in range(NH):
        tcopy(z, c, h, 2, partner).start()

    def wstep(s):
        for sgn in (-1, 1):
            src = z + sgn * s

            @pl.when((src >= 0) & (src <= 3))
            def _():
                with jax.named_scope("wzwait"):
                    wcopy(src, c, d, 0, up).wait_recv()

                @pl.when((z - sgn >= 0) & (z - sgn <= 3))
                def _():
                    wcopy(src, c, d, 0, (d, 2 * (z - sgn) + c)).start()

                for dd, path in side:
                    wcopy(src, c, d, path, (dd, t)).start()
                wcopy(src, c, d, 2, partner).start()

    def block(l1, l2, r1, r2, acc):
        a = _nt(l1, r1)
        g = _nt(l2, r2)
        h, da = _gelu_pair(a, g)
        acc[1, :, :] += _nn(h, r2)
        acc[0, :, :] += _nn(da, r1)

    elast = jnp.where(z == 0, 6, jnp.where(z == 3, 5, jnp.where(z == 1, 4, 3)))

    @pl.loop(0, 7)
    def _(e):
        s = (e + 1) // 2
        sgn = 1 - 2 * (e - 2 * (e // 2))
        src = z + sgn * s
        nxt = z - sgn

        @pl.when((e == 0) | (e == 1) | (e == 3))
        def _():
            wstep(jnp.where(e == 0, 1, jnp.where(e == 1, 2, 3)))

        @pl.when(e == 0)
        def _():
            town(NH // 2, NH)

        def epilogue():
            dgb[t] = jnp.zeros((8, D), jnp.float32)

            @pl.loop(0, TOK // RT)
            def _(i):
                r = pl.ds(pl.multiple_of(i * RT, RT), RT)
                x = xb[r, :].astype(jnp.float32)
                xh, rstd = _ln(x)
                dxn_ = yacc[0, r, :]
                p = dxn_ * xh
                dgb[t] += jnp.sum(p.reshape(RT // 8, 8, D), axis=0)
                dxh = dxn_ * g_ref[...].reshape(1, D)
                m1 = jnp.mean(dxh, axis=-1, keepdims=True)
                m2 = jnp.mean(dxh * xh, axis=-1, keepdims=True)
                h = i // (TH // RT)
                rr = pl.ds(pl.multiple_of((i - h * (TH // RT)) * RT, RT), RT)
                dyv = T[z, 1, h, c, rr, :].astype(jnp.float32)
                ob[r, :] = (dyv + rstd * (dxh - m1 - xh * m2)).astype(jnp.bfloat16)
                xb[r, :] = yacc[1, r, :].astype(jnp.bfloat16)

            pltpu.make_async_copy(xb, y_h, osem.at[0]).start()
            pltpu.make_async_copy(ob, dx_h, osem.at[1]).start()
            for k in range(1, 8):
                pltpu.make_async_remote_copy(
                    src_ref=dgb.at[t], dst_ref=dgb.at[t], send_sem=dgs.at[k],
                    recv_sem=dgr.at[k], device_id=(d, lax.rem(t + k, 8)),
                    device_id_type=MESH).start()

        def flush():
            with jax.named_scope("flush"):
                pltpu.make_async_copy(wacc.at[1], dw2_h, osem.at[3]).start()
                for i in range(FF // 128):
                    wt[:, i * 128:(i + 1) * 128] = wacc[0, i * 128:(i + 1) * 128, :].T
                pltpu.make_async_copy(wt, dw1_h, osem.at[2]).start()

        def wpart():
            @pl.when(e == 0)
            def _():
                wown(o).wait_recv()
                lo.wait()

            @pl.when(e > 0)
            def _():
                with jax.named_scope("wxywait"):
                    for dd, _p in side:
                        wcopy(src, c, dd, 2, partner).wait_recv()
                        wcopy(src, c, dd, 2, partner).start()
                with jax.named_scope("wd2dwait"):
                    for q in range(4):
                        wcopy(src, o, q, 2, partner).wait_recv()

            with jax.named_scope("tokside"):
                def fetch(i):
                    j = lax.rem(i, 2)
                    rr = pl.ds(pl.multiple_of(i * NB, NB), NB)
                    return pltpu.make_async_copy(W.at[src, :, rr, :], wb.at[j], bsem.at[j])

                fetch(0).start()

                @pl.loop(0, 2 * FF // NB)
                def _(i):
                    @pl.when(i + 1 < 2 * FF // NB)
                    def _():
                        fetch(i + 1).start()

                    fetch(i).wait()
                    j = lax.rem(i, 2)
                    block(T[z, 0, :, c].reshape(TOK, D), T[z, 1, :, c].reshape(TOK, D),
                          wb[j, 0], wb[j, 1], yacc)

            pl.when(e == elast)(epilogue)

        @pl.when((src >= 0) & (src <= 3))
        def _():
            @pl.loop(0, NH)
            def _(h):
                pl.when(h == NH // 2)(wpart)
                last = (e == elast) & (h == NH - 1)
                pl.when(last)(flush)

                @pl.when(e > 0)
                def _():
                    with jax.named_scope("tzwait"):
                        tcopy(src, c, h, 0, up).wait_recv()

                    @pl.when((nxt >= 0) & (nxt <= 3))
                    def _():
                        tcopy(src, c, h, 0, (d, 2 * nxt + c)).start()

                    tcopy(src, c, h, 2, partner).start()

                with jax.named_scope("td2dwait"):
                    tcopy(src, o, h, 2, partner).wait_recv()

                @pl.when(last)
                def _():
                    with jax.named_scope("tlast"):
                        cp = pltpu.make_async_copy(T.at[src, :, NH - 1], tl_h, osem.at[4])
                        cp.start()
                        cp.wait()

                @pl.when(jnp.logical_not(last))
                def _():
                    with jax.named_scope("fside"):
                        block(wo[0], wo[1], T[src, 0, h].reshape(2 * TH, D),
                              T[src, 1, h].reshape(2 * TH, D), wacc)

    for k in range(1, 8):
        pltpu.make_async_remote_copy(
            src_ref=dgb.at[t], dst_ref=dgb.at[t], send_sem=dgs.at[k],
            recv_sem=dgr.at[k], device_id=partner, device_id_type=MESH).wait_recv()
    dg_ref[...] = jnp.sum(jnp.sum(dgb[...], axis=0), axis=0)

    for k in range(1, 8):
        pltpu.make_async_remote_copy(
            src_ref=dgb.at[t], dst_ref=dgb.at[t], send_sem=dgs.at[k],
            recv_sem=dgr.at[k], device_id=partner, device_id_type=MESH).wait_send()
    wown(c).wait_send()

    @pl.when(z < 3)
    def _():
        wcopy(z, c, d, 0, up).wait_send()
        for h in range(NH):
            tcopy(z, c, h, 0, up).wait_send()

    @pl.when(z > 0)
    def _():
        wcopy(z, c, d, 1, down).wait_send()
        for h in range(NH):
            tcopy(z, c, h, 1, down).wait_send()

    for h in range(NH):
        tcopy(z, c, h, 2, partner).wait_send()

    @pl.loop(1, 7)
    def _(e):
        s = (e + 1) // 2
        sgn = 1 - 2 * (e - 2 * (e // 2))
        src = z + sgn * s
        nxt = z - sgn

        @pl.when((src >= 0) & (src <= 3))
        def _():
            @pl.when((nxt >= 0) & (nxt <= 3))
            def _():
                wcopy(src, c, d, 0, up).wait_send()
                for h in range(NH):
                    tcopy(src, c, h, 0, up).wait_send()

            for dd, path in side:
                wcopy(src, c, d, path, partner).wait_send()
                wcopy(src, c, dd, 2, partner).wait_send()
            wcopy(src, c, d, 2, partner).wait_send()
            for h in range(NH):
                tcopy(src, c, h, 2, partner).wait_send()

    pltpu.make_async_copy(xb, y_h, osem.at[0]).wait()
    pltpu.make_async_copy(ob, dx_h, osem.at[1]).wait()
    with jax.named_scope("owait"):
        pltpu.make_async_copy(wt, dw1_h, osem.at[2]).wait()
        pltpu.make_async_copy(wacc.at[1], dw2_h, osem.at[3]).wait()


def _finish(tl_h, w1_h, w2_h, p1_h, p2_h, yp_h, dxp_h, dgp_h, y_h, dx_h, dw1_h, dw2_h, dg_h,
            tl, w1, w2, a1, a2, yv, dxv, dgv, isem, osem):
    ins = [pltpu.make_async_copy(src, dst, isem.at[i]) for i, (src, dst) in enumerate(
        ((tl_h, tl), (w1_h, w1), (w2_h, w2), (p2_h, a2), (p1_h, a1), (yp_h, yv), (dxp_h, dxv), (dgp_h, dgv)))]
    for cp in ins:
        cp.start()
    ins[0].wait()
    xn = tl[0].reshape(2 * TH, D)
    dy = tl[1].reshape(2 * TH, D)
    ins[1].wait()
    a = _nn(xn, w1[...])
    ins[2].wait()
    g = _nt(dy, w2[...])
    h, da = _gelu_pair(a, g)
    outs = []

    def out(src, dst):
        cp = pltpu.make_async_copy(src, dst, osem.at[len(outs)])
        cp.start()
        outs.append(cp)

    for i, (src, dst) in ((5, (yv, y_h)), (6, (dxv, dx_h)), (7, (dgv, dg_h))):
        ins[i].wait()
        out(src, dst)
    ins[3].wait()
    for k in range(FF // 128):
        r = slice(k * 128, (k + 1) * 128)
        a2[r, :] += _tn(h[:, r], dy)
        out(a2.at[r, :], dw2_h.at[r, :])
    ins[4].wait()
    for k in range(D // 256):
        r = slice(k * 256, (k + 1) * 256)
        a1[r, :] += _tn(xn[:, r], da)
        out(a1.at[r, :], dw1_h.at[r, :])
    for cp in outs:
        cp.wait()


def solution(mesh):
    rows = P(("data", "tp"), None)
    bf, f32 = jnp.bfloat16, jnp.float32

    def body(X, gamma, W1, W2, dY):
        hbm = pl.BlockSpec(memory_space=pl.ANY)
        vm = pl.BlockSpec(memory_space=pltpu.VMEM)
        sd = jax.ShapeDtypeStruct
        dma = pltpu.SemaphoreType.DMA
        Yp, dXp, p1, p2, tl, _, dgp = pl.pallas_call(
            _kernel,
            name="mlp_gather",
            out_shape=(sd((TOK, D), bf), sd((TOK, D), bf), sd((D, FF), f32), sd((FF, D), f32),
                       sd((2, 2, TH, D), bf), sd((4, 2, 2 * FF, D), bf), sd((D,), f32)),
            in_specs=[hbm, vm, hbm, hbm, hbm],
            out_specs=[hbm] * 6 + [vm],
            scratch_shapes=[
                pltpu.VMEM((4, 2, NH, 2, TH, D), bf),
                pltpu.VMEM((2, FF, D), bf),
                pltpu.VMEM((2, 2, NB, D), bf),
                pltpu.VMEM((2, TOK, D), f32),
                pltpu.VMEM((2, FF, D), f32),
                pltpu.VMEM((D, FF), f32),
                pltpu.VMEM((TOK, D), bf),
                pltpu.VMEM((TOK, D), bf),
                pltpu.VMEM((8, 8, D), f32),
                pltpu.VMEM((D, FF), bf),
                dma((4 + NH,)),
                dma((5,)),
                dma((2,)),
                dma((4, NH, 3)),
                dma((4, 2, NH)),
                dma((4, 4, 6)),
                dma((4, 2, 4)),
                dma((8,)),
                dma((8,)),
            ],
            compiler_params=pltpu.CompilerParams(collective_id=0, has_side_effects=True, vmem_limit_bytes=VM1),
        )(X, gamma, W1, W2, dY)
        return pl.pallas_call(
            _finish,
            name="mlp_finish",
            out_shape=(sd((TOK, D), bf), sd((TOK, D), bf), sd((D, FF), f32), sd((FF, D), f32), sd((D,), f32)),
            in_specs=[hbm] * 8,
            out_specs=[hbm] * 5,
            scratch_shapes=[
                pltpu.VMEM((2, 2, TH, D), bf),
                pltpu.VMEM((D, FF), bf),
                pltpu.VMEM((FF, D), bf),
                pltpu.VMEM((D, FF), f32),
                pltpu.VMEM((FF, D), f32),
                pltpu.VMEM((TOK, D), bf),
                pltpu.VMEM((TOK, D), bf),
                pltpu.VMEM((D,), f32),
                dma((8,)),
                dma((13,)),
            ],
            compiler_params=pltpu.CompilerParams(vmem_limit_bytes=VM2),
        )(tl, W1, W2, p1, p2, Yp, dXp, dgp)

    return jax.shard_map(body, mesh=mesh,
                         in_specs=(rows, P(None), P(None, "tp"), P("tp", None), rows),
                         out_specs=(rows, rows, P("data", "tp"), rows, P("data")),
                         check_vma=False)
```

```python
import functools

import jax
import jax.numpy as jnp
from jax import lax
from jax.experimental import pallas as pl
from jax.experimental.pallas import tpu as pltpu
from jax.sharding import PartitionSpec as P

EPS = 1e-6
D = 1280
TOK = 512
FF = 640
NH = 4
TH = TOK // NH
NB = 256
RT = 64
STRIPS = ((0, 384), (384, 640))
VM1 = 60 * 2**20
VM2 = 60 * 2**20
K0 = 0.7978845608028654
K1 = 0.044715
MESH = pl.DeviceIdType.MESH


def _nt(a, b):
    return lax.dot_general(a, b, (((1,), (1,)), ((), ())), preferred_element_type=jnp.float32)


def _nn(a, b):
    return lax.dot_general(a, b, (((1,), (0,)), ((), ())), preferred_element_type=jnp.float32)


def _tn(a, b):
    return lax.dot_general(a, b, (((0,), (0,)), ((), ())), preferred_element_type=jnp.float32)


def _ln(x):
    mu = jnp.mean(x, axis=-1, keepdims=True)
    xc = x - mu
    var = jnp.mean(xc * xc, axis=-1, keepdims=True)
    rstd = lax.rsqrt(var + EPS)
    return xc * rstd, rstd


def _gelu_pair(a, g):
    a2 = a * a
    t = jnp.tanh(a * (K0 + (K0 * K1) * a2))
    cdf = 0.5 + 0.5 * t
    h = a * cdf
    dg = cdf + h * (1.0 - t) * (K0 + (3.0 * K0 * K1) * a2)
    return h.astype(jnp.bfloat16), (dg * g).astype(jnp.bfloat16)


def _kernel(x_h, g_ref, w1_h, w2_h, dy_h, y_h, dx_h, dw1_h, dw2_h, tl_h, W, dg_h, w1t_h,
            T, wo, wb, yacc, wacc, xb, ob, dgb, dgs8, dgo,
            w1n, lsem, osem, bsem, tsend, trecv, wsend, wrecv, dgs):
    d = lax.axis_index("data")
    t = lax.axis_index("tp")
    z = t // 2
    c = t - 2 * z
    o = 1 - c
    partner = (d, 2 * z + o)
    up = (d, 2 * z + 2 + c)
    down = (d, 2 * z - 2 + c)
    dxn = lax.rem(d + 2, 4)
    dyn = d + 1 - 2 * lax.rem(d, 2)
    ddg = 3 - d
    side = (dxn, dyn, ddg)

    def tslot(src, lane, h):
        return T.at[src, :, h, lane]

    def tcopy(src, lane, h, path, dev):
        s = tslot(src, lane, h)
        return pltpu.make_async_remote_copy(
            src_ref=s, dst_ref=s, send_sem=tsend.at[src, path],
            recv_sem=trecv.at[src, lane, h], device_id=dev, device_id_type=MESH)

    def tsent(src, path):
        s = T.at[src, :, :, c]
        pltpu.make_async_remote_copy(
            src_ref=s, dst_ref=s, send_sem=tsend.at[src, path],
            recv_sem=trecv.at[src, c, 0], device_id=partner, device_id_type=MESH).wait_send()

    def wcopy(src, lane, q, path, dev, n=1):
        s = W.at[src, :, pl.ds(pl.multiple_of(lane * FF + q * (FF // 4), 32), n * (FF // 4)), :]
        return pltpu.make_async_remote_copy(
            src_ref=s, dst_ref=s, send_sem=wsend.at[src, path],
            recv_sem=wrecv.at[src, (0, 0, 1, 2)[path]], device_id=dev, device_id_type=MESH)

    def wown(lane):
        return pltpu.make_async_remote_copy(
            src_ref=wo, dst_ref=W.at[z, :, pl.ds(pl.multiple_of(lane * FF, FF), FF), :], send_sem=wsend.at[z, 2],
            recv_sem=wrecv.at[z, 1], device_id=partner, device_id_type=MESH)

    frow = pl.ds(pl.multiple_of(c * FF, FF), FF)
    l1 = pltpu.make_async_copy(w1_h, w1n, lsem.at[0])
    l2 = pltpu.make_async_copy(w2_h, wo.at[1], lsem.at[1])
    l3 = pltpu.make_async_copy(x_h, xb, lsem.at[2])
    l1.start()
    l2.start()
    l3.start()
    l4 = [pltpu.make_async_copy(dy_h.at[pl.ds(h * TH, TH), :], T.at[z, 1, h, c], lsem.at[3 + h])
          for h in range(NH)]
    for cp in l4:
        cp.start()
    barrier = pltpu.get_barrier_semaphore()
    for k in range(1, 8):
        pl.semaphore_signal(barrier, inc=1, device_id=(d, lax.rem(t + k, 8)), device_id_type=MESH)
    for dd in side:
        pl.semaphore_signal(barrier, inc=1, device_id=(dd, t), device_id_type=MESH)
    pl.semaphore_wait(barrier, 10)

    def whalf(mat, path, dev):
        q = pl.ds(pl.multiple_of(d * (FF // 4), 32), FF // 4)
        return pltpu.make_async_remote_copy(
            src_ref=w2_h.at[q, :] if mat else wo.at[0, q, :],
            dst_ref=W.at[z, mat, pl.ds(pl.multiple_of(c * FF + d * (FF // 4), 32), FF // 4), :], send_sem=wsend.at[z, path],
            recv_sem=wrecv.at[z, 0], device_id=dev, device_id_type=MESH)

    @pl.when(z < 3)
    def _():
        whalf(1, 0, up).start()

    @pl.when(z > 0)
    def _():
        whalf(1, 1, down).start()

    l1.wait()

    for i in range(FF // 128):
        wo[0, i * 128:(i + 1) * 128, :] = w1n[:, i * 128:(i + 1) * 128].T

    l2.wait()
    l3.wait()

    @pl.loop(0, TOK // RT)
    def _(i):
        r = pl.ds(pl.multiple_of(i * RT, RT), RT)
        x = xb[r, :].astype(jnp.float32)
        xh, _ = _ln(x)
        h = i // (TH // RT)
        rr = pl.ds(pl.multiple_of((i - h * (TH // RT)) * RT, RT), RT)
        T[z, 0, h, c, rr, :] = (xh * g_ref[...].reshape(1, D)).astype(jnp.bfloat16)
        yacc[1, r, :] = x
        yacc[0, r, :] = jnp.zeros((RT, D), jnp.float32)

    @pl.when(z < 3)
    def _():
        whalf(0, 0, up).start()

    @pl.when(z > 0)
    def _():
        whalf(0, 1, down).start()

    wown(c).start()
    lo = pltpu.make_async_copy(wo, W.at[z, :, frow, :], lsem.at[3 + NH])
    lo.start()

    @pl.loop(0, FF // RT)
    def _(i):
        r = pl.ds(pl.multiple_of(i * RT, RT), RT)
        wacc[0, r, :] = jnp.zeros((RT, D), jnp.float32)
        wacc[1, r, :] = jnp.zeros((RT, D), jnp.float32)

    for cp in l4:
        cp.wait()

    def town(h0, h1):
        @pl.when(z < 3)
        def _():
            for h in range(h0, h1):
                tcopy(z, c, h, 0, up).start()

        @pl.when(z > 0)
        def _():
            for h in range(h0, h1):
                tcopy(z, c, h, 1, down).start()

    town(0, NH // 2)
    for h in range(NH):
        tcopy(z, c, h, 2, partner).start()

    def wstep(s):
        for sgn in (-1, 1):
            src = z + sgn * s

            @pl.when((src >= 0) & (src <= 3))
            def _():
                with jax.named_scope("wzwait"):
                    wcopy(src, c, d, 0, up).wait_recv()

                @pl.when((z - sgn >= 0) & (z - sgn <= 3))
                def _():
                    wcopy(src, c, d, 0, (d, 2 * (z - sgn) + c)).start()

                for dd in side:
                    wcopy(src, c, d, 3, (dd, t)).start()
                wcopy(src, c, d, 2, partner).start()

    def block(l1, l2, r1, r2, acc):
        a = _nt(l1, r1)
        g = _nt(l2, r2)
        h, da = _gelu_pair(a, g)
        acc[1, :, :] += _nn(h, r2)
        acc[0, :, :] += _nn(da, r1)

    elast = jnp.where(z == 0, 6, jnp.where(z == 3, 5, jnp.where(z == 1, 4, 3)))

    @pl.loop(0, 7)
    def _(e):
        s = (e + 1) // 2
        sgn = 1 - 2 * (e - 2 * (e // 2))
        src = z + sgn * s
        nxt = z - sgn

        @pl.when((e == 0) | (e == 1) | (e == 3))
        def _():
            wstep(jnp.where(e == 0, 1, jnp.where(e == 1, 2, 3)))

        @pl.when(e == 0)
        def _():
            town(NH // 2, NH)

        def epilogue():
            dgs8[...] = jnp.zeros((8, D), jnp.float32)

            @pl.loop(0, TOK // RT)
            def _(i):
                r = pl.ds(pl.multiple_of(i * RT, RT), RT)
                x = xb[r, :].astype(jnp.float32)
                xh, rstd = _ln(x)
                dxn_ = yacc[0, r, :]
                p = dxn_ * xh
                dgs8[...] += jnp.sum(p.reshape(RT // 8, 8, D), axis=0)
                dxh = dxn_ * g_ref[...].reshape(1, D)
                m1 = jnp.mean(dxh, axis=-1, keepdims=True)
                m2 = jnp.mean(dxh * xh, axis=-1, keepdims=True)
                h = i // (TH // RT)
                rr = pl.ds(pl.multiple_of((i - h * (TH // RT)) * RT, RT), RT)
                dyv = T[z, 1, h, c, rr, :].astype(jnp.float32)
                ob[r, :] = (dyv + rstd * (dxh - m1 - xh * m2)).astype(jnp.bfloat16)
                xb[r, :] = yacc[1, r, :].astype(jnp.bfloat16)

            dgb[t] = jnp.sum(dgs8[...], axis=0, keepdims=True)
            pltpu.make_async_copy(xb, y_h, osem.at[0]).start()
            pltpu.make_async_copy(ob, dx_h, osem.at[1]).start()
            for k in range(1, 8):
                pltpu.make_async_remote_copy(
                    src_ref=dgb.at[t], dst_ref=dgb.at[t], send_sem=dgs.at[0],
                    recv_sem=dgs.at[1], device_id=(d, lax.rem(t + k, 8)),
                    device_id_type=MESH).start()

        def flush():
            with jax.named_scope("flush"):
                pltpu.make_async_copy(wacc.at[1], dw2_h, osem.at[3]).start()
                pltpu.make_async_copy(wacc.at[0], dw1_h, osem.at[2]).start()
                pltpu.make_async_copy(wo.at[0], w1t_h, osem.at[6]).start()

        def wpart():
            @pl.when(e == 0)
            def _():
                wown(o).wait_recv()
                lo.wait()

            @pl.when(e > 0)
            def _():
                with jax.named_scope("wxywait"):
                    wcopy(src, c, 0, 3, partner, 3).wait_recv()
                    for dd in side:
                        wcopy(src, c, dd, 2, partner).start()
                with jax.named_scope("wd2dwait"):
                    wcopy(src, o, 0, 2, partner, 4).wait_recv()

            with jax.named_scope("tokside"):
                def fetch(i):
                    j = lax.rem(i, 2)
                    rr = pl.ds(pl.multiple_of(i * NB, NB), NB)
                    return pltpu.make_async_copy(W.at[src, :, rr, :], wb.at[j], bsem.at[j])

                fetch(0).start()

                @pl.loop(0, 2 * FF // NB)
                def _(i):
                    @pl.when(i + 1 < 2 * FF // NB)
                    def _():
                        fetch(i + 1).start()

                    fetch(i).wait()
                    j = lax.rem(i, 2)
                    block(T[z, 0, :, c].reshape(TOK, D), T[z, 1, :, c].reshape(TOK, D),
                          wb[j, 0], wb[j, 1], yacc)

            pl.when(e == elast)(epilogue)

        @pl.when((src >= 0) & (src <= 3))
        def _():
            @pl.loop(0, NH)
            def _(h):
                pl.when(h == NH // 2)(wpart)
                last = (e == elast) & (h == NH - 1)
                pl.when(last)(flush)

                @pl.when(e > 0)
                def _():
                    with jax.named_scope("tzwait"):
                        tcopy(src, c, h, 0, up).wait_recv()

                    @pl.when((nxt >= 0) & (nxt <= 3))
                    def _():
                        tcopy(src, c, h, 0, (d, 2 * nxt + c)).start()

                    tcopy(src, c, h, 2, partner).start()

                with jax.named_scope("td2dwait"):
                    tcopy(src, o, h, 2, partner).wait_recv()

                @pl.when(last)
                def _():
                    with jax.named_scope("tlast"):
                        pltpu.make_async_copy(T.at[src, :, NH - 1], tl_h, osem.at[4]).start()

                @pl.when(jnp.logical_not(last))
                def _():
                    with jax.named_scope("fside"):
                        block(wo[0], wo[1], T[src, 0, h].reshape(2 * TH, D),
                              T[src, 1, h].reshape(2 * TH, D), wacc)

    dgall = pltpu.make_async_remote_copy(
        src_ref=dgb.at[pl.ds(0, 7)], dst_ref=dgb.at[pl.ds(0, 7)], send_sem=dgs.at[0],
        recv_sem=dgs.at[1], device_id=partner, device_id_type=MESH)
    dgall.wait_recv()
    dgo[...] = jnp.sum(jnp.sum(dgb[...], axis=0), axis=0)
    dgc = pltpu.make_async_copy(dgo, dg_h, osem.at[5])
    dgc.start()

    dgall.wait_send()
    wown(c).wait_send()
    tsent(z, 2)

    @pl.when(z < 3)
    def _():
        wcopy(z, c, d, 0, up).wait_send()
        tsent(z, 0)

    @pl.when(z > 0)
    def _():
        wcopy(z, c, d, 1, down).wait_send()
        tsent(z, 1)

    @pl.loop(1, 7)
    def _(e):
        s = (e + 1) // 2
        sgn = 1 - 2 * (e - 2 * (e // 2))
        src = z + sgn * s
        nxt = z - sgn

        @pl.when((src >= 0) & (src <= 3))
        def _():
            @pl.when((nxt >= 0) & (nxt <= 3))
            def _():
                wcopy(src, c, d, 0, up).wait_send()
                tsent(src, 0)

            wcopy(src, c, 0, 3, partner, 3).wait_send()
            wcopy(src, c, 0, 2, partner, 4).wait_send()
            tsent(src, 2)

    with jax.named_scope("owait"):
        pltpu.make_async_copy(xb, y_h, osem.at[0]).wait()
        pltpu.make_async_copy(ob, dx_h, osem.at[1]).wait()
        pltpu.make_async_copy(T.at[z, :, NH - 1], tl_h, osem.at[4]).wait()
        dgc.wait()
        pltpu.make_async_copy(wacc.at[0], dw1_h, osem.at[2]).wait()
        pltpu.make_async_copy(wo.at[0], w1t_h, osem.at[6]).wait()
        pltpu.make_async_copy(wacc.at[1], dw2_h, osem.at[3]).wait()


def _finish(tl_h, w1_h, w2_h, p1_h, p2_h, yp_h, dxp_h, dgp_h, y_h, dx_h, dw1_h, dw2_h, dg_h,
            tl, w1, w2, a1, a2, o1, yv, dxv, dgv, isem, osem):
    ins = [pltpu.make_async_copy(src, dst, isem.at[i]) for i, (src, dst) in enumerate(
        ((tl_h, tl), (w1_h, w1), (w2_h, w2), (p2_h, a2), (p1_h, a1), (yp_h, yv), (dxp_h, dxv), (dgp_h, dgv)))]
    for cp in ins:
        cp.start()
    outs = []

    def out(src, dst):
        cp = pltpu.make_async_copy(src, dst, osem.at[len(outs)])
        cp.start()
        outs.append(cp)

    ins[0].wait()
    xn = tl[0].reshape(2 * TH, D)
    dy = tl[1].reshape(2 * TH, D)
    for n, (r0, r1) in enumerate(STRIPS):
        r = slice(r0, r1)
        if n == 0:
            ins[1].wait()
        a = _nt(w1[r, :], xn)
        if n == 0:
            ins[2].wait()
        g = _nt(w2[r, :], dy)
        h, da = _gelu_pair(a, g)
        if n == 0:
            ins[3].wait()
        a2[r, :] += _nn(h, dy)
        out(a2.at[r, :], dw2_h.at[r, :])
        if n == 0:
            ins[4].wait()
        a1[r, :] += _nn(da, xn)
        for k in range(r0, r1, 128):
            o1[:, k:k + 128] = a1[k:k + 128, :].T
        out(o1.at[:, r], dw1_h.at[:, r])
        if n == 0:
            for i, (src, dst) in ((5, (yv, y_h)), (6, (dxv, dx_h)), (7, (dgv, dg_h))):
                ins[i].wait()
                out(src, dst)
    for cp in outs:
        cp.wait()


def solution(mesh):
    rows = P(("data", "tp"), None)
    bf, f32 = jnp.bfloat16, jnp.float32

    def body(X, gamma, W1, W2, dY):
        hbm = pl.BlockSpec(memory_space=pl.ANY)
        vm = pl.BlockSpec(memory_space=pltpu.VMEM)
        sd = jax.ShapeDtypeStruct
        dma = pltpu.SemaphoreType.DMA
        Yp, dXp, p1, p2, tl, _, dgp, w1t = pl.pallas_call(
            _kernel,
            name="mlp_gather",
            out_shape=(sd((TOK, D), bf), sd((TOK, D), bf), sd((FF, D), f32), sd((FF, D), f32),
                       sd((2, 2, TH, D), bf), sd((4, 2, 2 * FF, D), bf), sd((D,), f32), sd((FF, D), bf)),
            in_specs=[hbm, vm, hbm, hbm, hbm],
            out_specs=[hbm] * 8,
            scratch_shapes=[
                pltpu.VMEM((4, 2, NH, 2, TH, D), bf),
                pltpu.VMEM((2, FF, D), bf),
                pltpu.VMEM((2, 2, NB, D), bf),
                pltpu.VMEM((2, TOK, D), f32),
                pltpu.VMEM((2, FF, D), f32),
                pltpu.VMEM((TOK, D), bf),
                pltpu.VMEM((TOK, D), bf),
                pltpu.VMEM((8, 1, D), f32),
                pltpu.VMEM((8, D), f32),
                pltpu.VMEM((D,), f32),
                pltpu.VMEM((D, FF), bf),
                dma((4 + NH,)),
                dma((7,)),
                dma((2,)),
                dma((4, 3)),
                dma((4, 2, NH)),
                dma((4, 4)),
                dma((4, 3)),
                dma((2,)),
            ],
            compiler_params=pltpu.CompilerParams(collective_id=0, has_side_effects=True, vmem_limit_bytes=VM1),
        )(X, gamma, W1, W2, dY)
        return pl.pallas_call(
            _finish,
            name="mlp_finish",
            out_shape=(sd((TOK, D), bf), sd((TOK, D), bf), sd((D, FF), f32), sd((FF, D), f32), sd((D,), f32)),
            in_specs=[hbm] * 8,
            out_specs=[hbm] * 5,
            scratch_shapes=[
                pltpu.VMEM((2, 2, TH, D), bf),
                pltpu.VMEM((FF, D), bf),
                pltpu.VMEM((FF, D), bf),
                pltpu.VMEM((FF, D), f32),
                pltpu.VMEM((FF, D), f32),
                pltpu.VMEM((D, FF), f32),
                pltpu.VMEM((TOK, D), bf),
                pltpu.VMEM((TOK, D), bf),
                pltpu.VMEM((D,), f32),
                dma((8,)),
                dma((3 + 2 * len(STRIPS),)),
            ],
            compiler_params=pltpu.CompilerParams(vmem_limit_bytes=VM2),
        )(tl, w1t, W2, p1, p2, Yp, dXp, dgp)

    return jax.shard_map(body, mesh=mesh,
                         in_specs=(rows, P(None), P(None, "tp"), P("tp", None), rows),
                         out_specs=(rows, rows, P("data", "tp"), rows, P("data")),
                         check_vma=False)
```

```python
import functools

import jax
import jax.numpy as jnp
from jax import lax
from jax.experimental import pallas as pl
from jax.experimental.pallas import tpu as pltpu
from jax.sharding import PartitionSpec as P

EPS = 1e-6
D = 1280
TOK = 512
FF = 640
NH = 4
TH = TOK // NH
NB = 256
RT = 64
STRIPS = ((0, 384), (384, 640))
VM1 = 42 * 2**20
VM2 = 20 * 2**20
K0 = 0.7978845608028654
K1 = 0.044715
MESH = pl.DeviceIdType.MESH


def _nt(a, b):
    return lax.dot_general(a, b, (((1,), (1,)), ((), ())), preferred_element_type=jnp.float32)


def _nn(a, b):
    return lax.dot_general(a, b, (((1,), (0,)), ((), ())), preferred_element_type=jnp.float32)


def _tn(a, b):
    return lax.dot_general(a, b, (((0,), (0,)), ((), ())), preferred_element_type=jnp.float32)


def _ln(x):
    mu = jnp.mean(x, axis=-1, keepdims=True)
    xc = x - mu
    var = jnp.mean(xc * xc, axis=-1, keepdims=True)
    rstd = lax.rsqrt(var + EPS)
    return xc * rstd, rstd


def _gelu_pair(a, g):
    a2 = a * a
    t = jnp.tanh(a * (K0 + (K0 * K1) * a2))
    cdf = 0.5 + 0.5 * t
    h = a * cdf
    dg = cdf + h * (1.0 - t) * (K0 + (3.0 * K0 * K1) * a2)
    return h.astype(jnp.bfloat16), (dg * g).astype(jnp.bfloat16)


def _kernel(x_h, g_h, w1_h, w2_h, dy_h, y_h, dx_h, p0, p1, p2, p3, p4, q0, q1, q2, q3, q4, tl_h, W, dg_h, w0_h, w1_o, w2_o, w3_h, w4_h,
            T, wo, wb, yacc, wacc, g_ref, dgb, dgs8, dgo,
            lsem, osem, bsem, tsend, trecv, wsend, wrecv, dgs):
    d = lax.axis_index("data")
    t = lax.axis_index("tp")
    z = t // 2
    c = t - 2 * z
    o = 1 - c
    partner = (d, 2 * z + o)
    up = (d, 2 * z + 2 + c)
    down = (d, 2 * z - 2 + c)
    dxn = lax.rem(d + 2, 4)
    dyn = d + 1 - 2 * lax.rem(d, 2)
    ddg = 3 - d
    side = (dxn, dyn, ddg)

    def tslot(src, lane, h):
        return T.at[src, :, h, lane]

    def tcopy(src, lane, h, path, dev):
        s = tslot(src, lane, h)
        return pltpu.make_async_remote_copy(
            src_ref=s, dst_ref=s, send_sem=tsend.at[src, path],
            recv_sem=trecv.at[src, lane, h], device_id=dev, device_id_type=MESH)

    def tsent(src, path):
        s = T.at[src, :, :, c]
        pltpu.make_async_remote_copy(
            src_ref=s, dst_ref=s, send_sem=tsend.at[src, path],
            recv_sem=trecv.at[src, c, 0], device_id=partner, device_id_type=MESH).wait_send()

    def wcopy(src, lane, q, path, dev, n=1):
        s = W.at[src, :, pl.ds(pl.multiple_of(lane * FF + q * (FF // 4), 32), n * (FF // 4)), :]
        return pltpu.make_async_remote_copy(
            src_ref=s, dst_ref=s, send_sem=wsend.at[src, path],
            recv_sem=wrecv.at[src, (0, 0, 1, 2)[path]], device_id=dev, device_id_type=MESH)

    def wown(lane):
        return pltpu.make_async_remote_copy(
            src_ref=wo, dst_ref=W.at[z, :, pl.ds(pl.multiple_of(lane * FF, FF), FF), :], send_sem=wsend.at[z, 2],
            recv_sem=wrecv.at[z, 1], device_id=partner, device_id_type=MESH)

    barrier = pltpu.get_barrier_semaphore()

    def greet(dev):
        pl.semaphore_signal(barrier, inc=1, device_id=dev, device_id_type=MESH)

    pl.when(z < 3)(lambda: greet(up))
    pl.when(z > 0)(lambda: greet(down))
    greet(partner)
    for dd in side:
        greet((dd, t))

    frow = pl.ds(pl.multiple_of(c * FF, FF), FF)
    w1b = [wb.at[i // 4, (i // 2) % 2, :, (i % 2) * FF:(i % 2 + 1) * FF] for i in range(D // NB)]
    l1 = [pltpu.make_async_copy(w1_h.at[i * NB:(i + 1) * NB, :], w1b[i], lsem.at[4 + 2 * NH + i])
          for i in range(D // NB)]
    l2 = pltpu.make_async_copy(w2_h, wo.at[1], lsem.at[1])
    for cp in l1:
        cp.start()
    l2.start()
    l3 = [pltpu.make_async_copy(x_h.at[pl.ds(h * TH, TH), :], T.at[z, 0, h, c], lsem.at[4 + NH + h])
          for h in range(NH)]
    for cp in l3:
        cp.start()
    lg = pltpu.make_async_copy(g_h, g_ref, lsem.at[0])
    lg.start()
    l4 = [pltpu.make_async_copy(dy_h.at[pl.ds(h * TH, TH), :], T.at[z, 1, h, c], lsem.at[3 + h])
          for h in range(NH)]
    for cp in l4:
        cp.start()
    pl.semaphore_wait(barrier, 4 + (z > 0).astype(jnp.int32) + (z < 3).astype(jnp.int32))

    def whalf(mat, path, dev):
        q = pl.ds(pl.multiple_of(d * (FF // 4), 32), FF // 4)
        return pltpu.make_async_remote_copy(
            src_ref=w2_h.at[q, :] if mat else wo.at[0, q, :],
            dst_ref=W.at[z, mat, pl.ds(pl.multiple_of(c * FF + d * (FF // 4), 32), FF // 4), :], send_sem=wsend.at[z, path],
            recv_sem=wrecv.at[z, 0], device_id=dev, device_id_type=MESH)

    @pl.when(z < 3)
    def _():
        whalf(1, 0, up).start()

    @pl.when(z > 0)
    def _():
        whalf(1, 1, down).start()

    for i in range(D // NB):
        l1[i].wait()
        wo[0, :, i * NB:(i + 1) * NB] = w1b[i][...].T

    l2.wait()
    lg.wait()
    for cp in l3:
        cp.wait()

    @pl.loop(0, TOK // RT)
    def _(i):
        r = pl.ds(pl.multiple_of(i * RT, RT), RT)
        h = i // (TH // RT)
        rr = pl.ds(pl.multiple_of((i - h * (TH // RT)) * RT, RT), RT)
        x = T[z, 0, h, c, rr, :].astype(jnp.float32)
        xh, _ = _ln(x)
        T[z, 0, h, c, rr, :] = (xh * g_ref[...].reshape(1, D)).astype(jnp.bfloat16)
        yacc[1, r, :] = x
        yacc[0, r, :] = jnp.zeros((RT, D), jnp.float32)

    @pl.when(z < 3)
    def _():
        whalf(0, 0, up).start()

    @pl.when(z > 0)
    def _():
        whalf(0, 1, down).start()

    wown(c).start()
    lo = pltpu.make_async_copy(wo, W.at[z, :, frow, :], lsem.at[3 + NH])
    lo.start()

    @pl.loop(0, FF // RT)
    def _(i):
        r = pl.ds(pl.multiple_of(i * RT, RT), RT)
        wacc[0, r, :] = jnp.zeros((RT, D), jnp.float32)
        wacc[1, r, :] = jnp.zeros((RT, D), jnp.float32)

    for cp in l4:
        cp.wait()

    def town(h0, h1):
        @pl.when(z < 3)
        def _():
            for h in range(h0, h1):
                tcopy(z, c, h, 0, up).start()

        @pl.when(z > 0)
        def _():
            for h in range(h0, h1):
                tcopy(z, c, h, 1, down).start()

    town(0, NH // 2)
    for h in range(NH):
        tcopy(z, c, h, 2, partner).start()

    def wstep(s):
        for sgn in (-1, 1):
            src = z + sgn * s

            @pl.when((src >= 0) & (src <= 3))
            def _():
                with jax.named_scope("wzwait"):
                    wcopy(src, c, d, 0, up).wait_recv()

                @pl.when((z - sgn >= 0) & (z - sgn <= 3))
                def _():
                    wcopy(src, c, d, 0, (d, 2 * (z - sgn) + c)).start()

                for dd in side:
                    wcopy(src, c, d, 3, (dd, t)).start()
                wcopy(src, c, d, 2, partner).start()

    def block(l1, l2, r1, r2, acc):
        a = _nt(l1, r1)
        g = _nt(l2, r2)
        h, da = _gelu_pair(a, g)
        acc[1, :, :] += _nn(h, r2)
        acc[0, :, :] += _nn(da, r1)

    elast = jnp.where(z == 0, 6, jnp.where(z == 3, 5, jnp.where(z == 1, 4, 3)))

    @pl.loop(0, 7)
    def _(e):
        s = (e + 1) // 2
        sgn = 1 - 2 * (e - 2 * (e // 2))
        src = z + sgn * s
        nxt = z - sgn

        @pl.when((e == 0) | (e == 1) | (e == 3))
        def _():
            wstep(jnp.where(e == 0, 1, jnp.where(e == 1, 2, 3)))

        @pl.when(e == 0)
        def _():
            town(NH // 2, NH)

        def xcopy(n):
            return pltpu.make_async_copy(x_h.at[n * NB:(n + 1) * NB, :], wb.at[0, n], bsem.at[n])

        def epilogue():
            for n in range(2):
                xcopy(n).start()
            for n in range(2):
                xcopy(n).wait()
            dgs8[...] = jnp.zeros((8, D), jnp.float32)

            @pl.loop(0, TOK // RT)
            def _(i):
                r = pl.ds(pl.multiple_of(i * RT, RT), RT)
                n = i // (NB // RT)
                wr = pl.ds(pl.multiple_of((i - n * (NB // RT)) * RT, RT), RT)
                x = wb[0, n, wr, :].astype(jnp.float32)
                xh, rstd = _ln(x)
                dxn_ = yacc[0, r, :]
                p = dxn_ * xh
                dgs8[...] += jnp.sum(p.reshape(RT // 8, 8, D), axis=0)
                dxh = dxn_ * g_ref[...].reshape(1, D)
                m1 = jnp.mean(dxh, axis=-1, keepdims=True)
                m2 = jnp.mean(dxh * xh, axis=-1, keepdims=True)
                h = i // (TH // RT)
                rr = pl.ds(pl.multiple_of((i - h * (TH // RT)) * RT, RT), RT)
                dyv = T[z, 1, h, c, rr, :].astype(jnp.float32)
                wb[0, n, wr, :] = (dyv + rstd * (dxh - m1 - xh * m2)).astype(jnp.bfloat16)
                wb[1, n, wr, :] = yacc[1, r, :].astype(jnp.bfloat16)

            dgb[t] = jnp.sum(dgs8[...], axis=0, keepdims=True)
            for n in range(2):
                pltpu.make_async_copy(wb.at[1, n], y_h.at[n * NB:(n + 1) * NB, :], osem.at[2 * n]).start()
                pltpu.make_async_copy(wb.at[0, n], dx_h.at[n * NB:(n + 1) * NB, :], osem.at[2 * n + 1]).start()
            for k in range(1, 8):
                pltpu.make_async_remote_copy(
                    src_ref=dgb.at[t], dst_ref=dgb.at[t], send_sem=dgs.at[0],
                    recv_sem=dgs.at[1], device_id=(d, lax.rem(t + k, 8)),
                    device_id_type=MESH).start()

        def flush():
            with jax.named_scope("flush"):
                for i in range(5):
                    pltpu.make_async_copy(wacc.at[1, i * 128:(i + 1) * 128, :], (q0, q1, q2, q3, q4)[i], osem.at[7]).start()
                for i in range(5):
                    pltpu.make_async_copy(wacc.at[0, i * 128:(i + 1) * 128, :], (p0, p1, p2, p3, p4)[i], osem.at[8]).start()
                for i in range(5):
                    pltpu.make_async_copy(wo.at[0, i * 128:(i + 1) * 128, :], (w0_h, w1_o, w2_o, w3_h, w4_h)[i],
                                          osem.at[6]).start()

        def wpart():
            @pl.when(e == 0)
            def _():
                wown(o).wait_recv()
                lo.wait()

            @pl.when(e > 0)
            def _():
                with jax.named_scope("wxywait"):
                    wcopy(src, c, 0, 3, partner, 3).wait_recv()
                    for dd in side:
                        wcopy(src, c, dd, 2, partner).start()
                with jax.named_scope("wd2dwait"):
                    wcopy(src, o, 0, 2, partner, 4).wait_recv()

            with jax.named_scope("tokside"):
                def fetch(i):
                    j = lax.rem(i, 2)
                    rr = pl.ds(pl.multiple_of(i * NB, NB), NB)
                    return pltpu.make_async_copy(W.at[src, :, rr, :], wb.at[j], bsem.at[j])

                fetch(0).start()

                @pl.loop(0, 2 * FF // NB)
                def _(i):
                    @pl.when(i + 1 < 2 * FF // NB)
                    def _():
                        fetch(i + 1).start()

                    fetch(i).wait()
                    j = lax.rem(i, 2)
                    block(T[z, 0, :, c].reshape(TOK, D), T[z, 1, :, c].reshape(TOK, D),
                          wb[j, 0], wb[j, 1], yacc)

            pl.when(e == elast)(epilogue)

        @pl.when((src >= 0) & (src <= 3))
        def _():
            @pl.loop(0, NH)
            def _(h):
                pl.when(h == jnp.where(e == elast, 0, NH // 2))(wpart)
                last = (e == elast) & (h == NH - 1)
                pl.when(last)(flush)

                @pl.when(e > 0)
                def _():
                    with jax.named_scope("tzwait"):
                        tcopy(src, c, h, 0, up).wait_recv()

                    @pl.when((nxt >= 0) & (nxt <= 3))
                    def _():
                        tcopy(src, c, h, 0, (d, 2 * nxt + c)).start()

                    tcopy(src, c, h, 2, partner).start()

                with jax.named_scope("td2dwait"):
                    tcopy(src, o, h, 2, partner).wait_recv()

                @pl.when(last)
                def _():
                    with jax.named_scope("tlast"):
                        pltpu.make_async_copy(T.at[src, :, NH - 1], tl_h, osem.at[4]).start()

                @pl.when(jnp.logical_not(last))
                def _():
                    with jax.named_scope("fside"):
                        block(wo[0], wo[1], T[src, 0, h].reshape(2 * TH, D),
                              T[src, 1, h].reshape(2 * TH, D), wacc)

    dgall = pltpu.make_async_remote_copy(
        src_ref=dgb.at[pl.ds(0, 7)], dst_ref=dgb.at[pl.ds(0, 7)], send_sem=dgs.at[0],
        recv_sem=dgs.at[1], device_id=partner, device_id_type=MESH)
    dgall.wait_recv()
    dgo[...] = jnp.sum(jnp.sum(dgb[...], axis=0), axis=0)
    dgc = pltpu.make_async_copy(dgo, dg_h, osem.at[5])
    dgc.start()

    dgall.wait_send()
    wown(c).wait_send()
    tsent(z, 2)

    @pl.when(z < 3)
    def _():
        wcopy(z, c, d, 0, up).wait_send()
        tsent(z, 0)

    @pl.when(z > 0)
    def _():
        wcopy(z, c, d, 1, down).wait_send()
        tsent(z, 1)

    @pl.loop(1, 7)
    def _(e):
        s = (e + 1) // 2
        sgn = 1 - 2 * (e - 2 * (e // 2))
        src = z + sgn * s
        nxt = z - sgn

        @pl.when((src >= 0) & (src <= 3))
        def _():
            @pl.when((nxt >= 0) & (nxt <= 3))
            def _():
                wcopy(src, c, d, 0, up).wait_send()
                tsent(src, 0)

            wcopy(src, c, 0, 3, partner, 3).wait_send()
            wcopy(src, c, 0, 2, partner, 4).wait_send()
            tsent(src, 2)

    with jax.named_scope("owait"):
        for n in range(2):
            pltpu.make_async_copy(wb.at[1, n], y_h.at[n * NB:(n + 1) * NB, :], osem.at[2 * n]).wait()
            pltpu.make_async_copy(wb.at[0, n], dx_h.at[n * NB:(n + 1) * NB, :], osem.at[2 * n + 1]).wait()
        pltpu.make_async_copy(T.at[z, :, NH - 1], tl_h, osem.at[4]).wait()
        dgc.wait()
        pltpu.make_async_copy(wacc.at[0], wacc.at[0], osem.at[8]).wait()
        pltpu.make_async_copy(wo.at[0], wo.at[0], osem.at[6]).wait()
        pltpu.make_async_copy(wacc.at[1], wacc.at[1], osem.at[7]).wait()


def _finish(tl, w2, *refs):
    p1, p2, w1 = refs[:5], refs[5:10], refs[10:15]
    yv, dxv, dgv, y_h, dx_h, dw1_h, dw2_h, dg_h, o1, o2, osem = refs[15:]
    outs = []

    def out(src, dst):
        cp = pltpu.make_async_copy(src, dst, osem.at[len(outs)])
        cp.start()
        outs.append(cp)

    out(yv, y_h)
    out(dxv, dx_h)
    out(dgv, dg_h)
    xn = tl[0].reshape(2 * TH, D)
    dy = tl[1].reshape(2 * TH, D)
    for r0, r1 in STRIPS:
        r = slice(r0, r1)
        a = _nt(jnp.concatenate([w1[k // 128][...] for k in range(r0, r1, 128)], axis=0), xn)
        g = _nt(w2[r, :], dy)
        h, da = _gelu_pair(a, g)
        q = _nn(h, dy)
        for k in range(r0, r1, 128):
            o2[k:k + 128, :] = p2[k // 128][...] + q[k - r0:k - r0 + 128, :]
        out(o2.at[r, :], dw2_h.at[r, :])
        q = _nn(da, xn)
        for k in range(r0, r1, 128):
            o1[:, k:k + 128] = (p1[k // 128][...] + q[k - r0:k - r0 + 128, :]).T
        out(o1.at[:, r], dw1_h.at[:, r])
    for cp in outs:
        cp.wait()


def solution(mesh):
    rows = P(("data", "tp"), None)
    bf, f32 = jnp.bfloat16, jnp.float32

    def body(X, gamma, W1, W2, dY):
        hbm = pl.BlockSpec(memory_space=pl.ANY)
        vm = pl.BlockSpec(memory_space=pltpu.VMEM)
        sd = jax.ShapeDtypeStruct
        dma = pltpu.SemaphoreType.DMA
        Yp, dXp, *pq = pl.pallas_call(
            _kernel,
            name="mlp_gather",
            out_shape=(sd((TOK, D), bf), sd((TOK, D), bf), *[sd((128, D), f32)] * 10,
                       sd((2, 2, TH, D), bf), sd((4, 2, 2 * FF, D), bf), sd((D,), f32), *[sd((128, D), bf)] * 5),
            in_specs=[hbm] * 5,
            out_specs=[hbm] * 20,
            scratch_shapes=[
                pltpu.VMEM((4, 2, NH, 2, TH, D), bf),
                pltpu.VMEM((2, FF, D), bf),
                pltpu.VMEM((2, 2, NB, D), bf),
                pltpu.VMEM((2, TOK, D), f32),
                pltpu.VMEM((2, FF, D), f32),
                pltpu.VMEM((D,), f32),
                pltpu.VMEM((8, 1, D), f32),
                pltpu.VMEM((8, D), f32),
                pltpu.VMEM((D,), f32),
                dma((4 + 2 * NH + D // NB,)),
                dma((9,)),
                dma((2,)),
                dma((4, 3)),
                dma((4, 2, NH)),
                dma((4, 4)),
                dma((4, 3)),
                dma((2,)),
            ],
            compiler_params=pltpu.CompilerParams(collective_id=0, has_side_effects=True, vmem_limit_bytes=VM1),
        )(X, gamma, W1, W2, dY)
        return pl.pallas_call(
            _finish,
            name="mlp_finish",
            out_shape=(sd((TOK, D), bf), sd((TOK, D), bf), sd((D, FF), f32), sd((FF, D), f32), sd((D,), f32)),
            in_specs=[vm] * 20,
            out_specs=[hbm] * 5,
            scratch_shapes=[
                pltpu.VMEM((D, FF), f32),
                pltpu.VMEM((FF, D), f32),
                dma((3 + 2 * len(STRIPS),)),
            ],
            compiler_params=pltpu.CompilerParams(vmem_limit_bytes=VM2),
        )(pq[10], W2, *pq[:10], *pq[13:], Yp, dXp, pq[12])

    return jax.shard_map(body, mesh=mesh,
                         in_specs=(rows, P(None), P(None, "tp"), P("tp", None), rows),
                         out_specs=(rows, rows, P("data", "tp"), rows, P("data")),
                         check_vma=False)
```

```python
import functools

import jax
import jax.numpy as jnp
from jax import lax
from jax.experimental import pallas as pl
from jax.experimental.pallas import tpu as pltpu
from jax.sharding import PartitionSpec as P

EPS = 1e-6
D = 1280
TOK = 512
FF = 640
NH = 4
TH = TOK // NH
NB = 256
RT = 64
STRIPS = ((0, 256), (256, 512), (512, 640))
VM1 = 42 * 2**20
VM2 = 20 * 2**20
K0 = 0.7978845608028654
K1 = 0.044715
MESH = pl.DeviceIdType.MESH


def _nt(a, b):
    return lax.dot_general(a, b, (((1,), (1,)), ((), ())), preferred_element_type=jnp.float32)


def _nn(a, b):
    return lax.dot_general(a, b, (((1,), (0,)), ((), ())), preferred_element_type=jnp.float32)


def _tn(a, b):
    return lax.dot_general(a, b, (((0,), (0,)), ((), ())), preferred_element_type=jnp.float32)


def _ln(x):
    mu = jnp.mean(x, axis=-1, keepdims=True)
    xc = x - mu
    var = jnp.mean(xc * xc, axis=-1, keepdims=True)
    rstd = lax.rsqrt(var + EPS)
    return xc * rstd, rstd


def _gelu_pair(a, g):
    a2 = a * a
    t = jnp.tanh(a * (K0 + (K0 * K1) * a2))
    cdf = 0.5 + 0.5 * t
    h = a * cdf
    dg = cdf + h * (1.0 - t) * (K0 + (3.0 * K0 * K1) * a2)
    return h.astype(jnp.bfloat16), (dg * g).astype(jnp.bfloat16)


def _kernel(x_h, g_h, w1_h, w2_h, dy_h, y_h, dx_h, p0, p1, p2, p3, p4, q0, q1, q2, q3, q4, tl_h, W, dg_h, w0_h, w1_o, w2_o, w3_h, w4_h,
            T, wo, wb, yacc, wacc, g_ref, dgb, dgs8, dgo,
            lsem, osem, bsem, tsend, trecv, wsend, wrecv, dgs):
    d = lax.axis_index("data")
    t = lax.axis_index("tp")
    z = t // 2
    c = t - 2 * z
    o = 1 - c
    partner = (d, 2 * z + o)
    up = (d, 2 * z + 2 + c)
    down = (d, 2 * z - 2 + c)
    dxn = lax.rem(d + 2, 4)
    dyn = d + 1 - 2 * lax.rem(d, 2)
    ddg = 3 - d
    side = (dxn, dyn, ddg)

    def tslot(src, lane, h):
        return T.at[src, :, h, lane]

    def tcopy(src, lane, h, path, dev):
        s = tslot(src, lane, h)
        return pltpu.make_async_remote_copy(
            src_ref=s, dst_ref=s, send_sem=tsend.at[src, path],
            recv_sem=trecv.at[src, lane, h], device_id=dev, device_id_type=MESH)

    def tsent(src, path):
        s = T.at[src, :, :, c]
        pltpu.make_async_remote_copy(
            src_ref=s, dst_ref=s, send_sem=tsend.at[src, path],
            recv_sem=trecv.at[src, c, 0], device_id=partner, device_id_type=MESH).wait_send()

    def wcopy(src, lane, q, path, dev, n=1):
        s = W.at[src, :, pl.ds(pl.multiple_of(lane * FF + q * (FF // 4), 32), n * (FF // 4)), :]
        return pltpu.make_async_remote_copy(
            src_ref=s, dst_ref=s, send_sem=wsend.at[src, path],
            recv_sem=wrecv.at[src, (0, 0, 1, 2)[path]], device_id=dev, device_id_type=MESH)

    def wown(lane):
        return pltpu.make_async_remote_copy(
            src_ref=wo, dst_ref=W.at[z, :, pl.ds(pl.multiple_of(lane * FF, FF), FF), :], send_sem=wsend.at[z, 2],
            recv_sem=wrecv.at[z, 1], device_id=partner, device_id_type=MESH)

    barrier = pltpu.get_barrier_semaphore()

    def greet(dev):
        pl.semaphore_signal(barrier, inc=1, device_id=dev, device_id_type=MESH)

    pl.when(z < 3)(lambda: greet(up))
    pl.when(z > 0)(lambda: greet(down))
    greet(partner)
    for dd in side:
        greet((dd, t))

    frow = pl.ds(pl.multiple_of(c * FF, FF), FF)
    w1b = [wb.at[i // 4, (i // 2) % 2, :, (i % 2) * FF:(i % 2 + 1) * FF] for i in range(D // NB)]
    l1 = [pltpu.make_async_copy(w1_h.at[i * NB:(i + 1) * NB, :], w1b[i], lsem.at[4 + 2 * NH + i])
          for i in range(D // NB)]
    l2 = pltpu.make_async_copy(w2_h, wo.at[1], lsem.at[1])
    for cp in l1:
        cp.start()
    l2.start()
    l3 = [pltpu.make_async_copy(x_h.at[pl.ds(h * TH, TH), :], T.at[z, 0, h, c], lsem.at[4 + NH + h])
          for h in range(NH)]
    for cp in l3:
        cp.start()
    lg = pltpu.make_async_copy(g_h, g_ref, lsem.at[0])
    lg.start()
    l4 = [pltpu.make_async_copy(dy_h.at[pl.ds(h * TH, TH), :], T.at[z, 1, h, c], lsem.at[3 + h])
          for h in range(NH)]
    for cp in l4:
        cp.start()
    pl.semaphore_wait(barrier, 4 + (z > 0).astype(jnp.int32) + (z < 3).astype(jnp.int32))

    def whalf(mat, path, dev):
        q = pl.ds(pl.multiple_of(d * (FF // 4), 32), FF // 4)
        return pltpu.make_async_remote_copy(
            src_ref=w2_h.at[q, :] if mat else wo.at[0, q, :],
            dst_ref=W.at[z, mat, pl.ds(pl.multiple_of(c * FF + d * (FF // 4), 32), FF // 4), :], send_sem=wsend.at[z, path],
            recv_sem=wrecv.at[z, 0], device_id=dev, device_id_type=MESH)

    @pl.when(z < 3)
    def _():
        whalf(1, 0, up).start()

    @pl.when(z > 0)
    def _():
        whalf(1, 1, down).start()

    for i in range(D // NB):
        l1[i].wait()
        wo[0, :, i * NB:(i + 1) * NB] = w1b[i][...].T

    l2.wait()
    lg.wait()
    for cp in l3:
        cp.wait()

    @pl.loop(0, TOK // RT)
    def _(i):
        r = pl.ds(pl.multiple_of(i * RT, RT), RT)
        h = i // (TH // RT)
        rr = pl.ds(pl.multiple_of((i - h * (TH // RT)) * RT, RT), RT)
        x = T[z, 0, h, c, rr, :].astype(jnp.float32)
        xh, _ = _ln(x)
        T[z, 0, h, c, rr, :] = (xh * g_ref[...].reshape(1, D)).astype(jnp.bfloat16)
        yacc[1, r, :] = x
        yacc[0, r, :] = jnp.zeros((RT, D), jnp.float32)

    @pl.when(z < 3)
    def _():
        whalf(0, 0, up).start()

    @pl.when(z > 0)
    def _():
        whalf(0, 1, down).start()

    wown(c).start()
    lo = pltpu.make_async_copy(wo, W.at[z, :, frow, :], lsem.at[3 + NH])
    lo.start()

    @pl.loop(0, FF // RT)
    def _(i):
        r = pl.ds(pl.multiple_of(i * RT, RT), RT)
        wacc[0, r, :] = jnp.zeros((RT, D), jnp.float32)
        wacc[1, r, :] = jnp.zeros((RT, D), jnp.float32)

    for cp in l4:
        cp.wait()

    def town(h0, h1):
        @pl.when(z < 3)
        def _():
            for h in range(h0, h1):
                tcopy(z, c, h, 0, up).start()

        @pl.when(z > 0)
        def _():
            for h in range(h0, h1):
                tcopy(z, c, h, 1, down).start()

    town(0, NH // 2)
    for h in range(NH):
        tcopy(z, c, h, 2, partner).start()

    def wstep(s):
        for sgn in (-1, 1):
            src = z + sgn * s

            @pl.when((src >= 0) & (src <= 3))
            def _():
                with jax.named_scope("wzwait"):
                    wcopy(src, c, d, 0, up).wait_recv()

                @pl.when((z - sgn >= 0) & (z - sgn <= 3))
                def _():
                    wcopy(src, c, d, 0, (d, 2 * (z - sgn) + c)).start()

                for dd in side:
                    wcopy(src, c, d, 3, (dd, t)).start()
                wcopy(src, c, d, 2, partner).start()

    def block(l1, l2, r1, r2, acc):
        a = _nt(l1, r1)
        g = _nt(l2, r2)
        h, da = _gelu_pair(a, g)
        acc[1, :, :] += _nn(h, r2)
        acc[0, :, :] += _nn(da, r1)

    elast = jnp.where(z == 0, 6, jnp.where(z == 3, 5, jnp.where(z == 1, 4, 3)))

    @pl.loop(0, 7)
    def _(e):
        s = (e + 1) // 2
        sgn = 1 - 2 * (e - 2 * (e // 2))
        src = z + sgn * s
        nxt = z - sgn

        @pl.when((e == 0) | (e == 1) | (e == 3))
        def _():
            wstep(jnp.where(e == 0, 1, jnp.where(e == 1, 2, 3)))

        @pl.when(e == 0)
        def _():
            town(NH // 2, NH)

        def xcopy(n):
            return pltpu.make_async_copy(x_h.at[n * NB:(n + 1) * NB, :], wb.at[0, n], bsem.at[n])

        def epilogue():
            for n in range(2):
                xcopy(n).start()
            for n in range(2):
                xcopy(n).wait()
            dgs8[...] = jnp.zeros((8, D), jnp.float32)

            @pl.loop(0, TOK // RT)
            def _(i):
                r = pl.ds(pl.multiple_of(i * RT, RT), RT)
                n = i // (NB // RT)
                wr = pl.ds(pl.multiple_of((i - n * (NB // RT)) * RT, RT), RT)
                x = wb[0, n, wr, :].astype(jnp.float32)
                xh, rstd = _ln(x)
                dxn_ = yacc[0, r, :]
                p = dxn_ * xh
                dgs8[...] += jnp.sum(p.reshape(RT // 8, 8, D), axis=0)
                dxh = dxn_ * g_ref[...].reshape(1, D)
                m1 = jnp.mean(dxh, axis=-1, keepdims=True)
                m2 = jnp.mean(dxh * xh, axis=-1, keepdims=True)
                h = i // (TH // RT)
                rr = pl.ds(pl.multiple_of((i - h * (TH // RT)) * RT, RT), RT)
                dyv = T[z, 1, h, c, rr, :].astype(jnp.float32)
                wb[0, n, wr, :] = (dyv + rstd * (dxh - m1 - xh * m2)).astype(jnp.bfloat16)
                wb[1, n, wr, :] = yacc[1, r, :].astype(jnp.bfloat16)

            dgb[t] = jnp.sum(dgs8[...], axis=0, keepdims=True)
            for n in range(2):
                pltpu.make_async_copy(wb.at[1, n], y_h.at[n * NB:(n + 1) * NB, :], osem.at[2 * n]).start()
                pltpu.make_async_copy(wb.at[0, n], dx_h.at[n * NB:(n + 1) * NB, :], osem.at[2 * n + 1]).start()
            for k in range(1, 8):
                pltpu.make_async_remote_copy(
                    src_ref=dgb.at[t], dst_ref=dgb.at[t], send_sem=dgs.at[0],
                    recv_sem=dgs.at[1], device_id=(d, lax.rem(t + k, 8)),
                    device_id_type=MESH).start()

        def flush():
            with jax.named_scope("flush"):
                for i in range(5):
                    pltpu.make_async_copy(wacc.at[1, i * 128:(i + 1) * 128, :], (q0, q1, q2, q3, q4)[i], osem.at[7]).start()
                for i in range(5):
                    pltpu.make_async_copy(wacc.at[0, i * 128:(i + 1) * 128, :], (p0, p1, p2, p3, p4)[i], osem.at[8]).start()
                for i in range(5):
                    pltpu.make_async_copy(wo.at[0, i * 128:(i + 1) * 128, :], (w0_h, w1_o, w2_o, w3_h, w4_h)[i],
                                          osem.at[6]).start()

        def wpart():
            @pl.when(e == 0)
            def _():
                wown(o).wait_recv()
                lo.wait()

            @pl.when(e > 0)
            def _():
                with jax.named_scope("wxywait"):
                    wcopy(src, c, 0, 3, partner, 3).wait_recv()
                    for dd in side:
                        wcopy(src, c, dd, 2, partner).start()
                with jax.named_scope("wd2dwait"):
                    wcopy(src, o, 0, 2, partner, 4).wait_recv()

            with jax.named_scope("tokside"):
                def fetch(i):
                    j = lax.rem(i, 2)
                    rr = pl.ds(pl.multiple_of(i * NB, NB), NB)
                    return pltpu.make_async_copy(W.at[src, :, rr, :], wb.at[j], bsem.at[j])

                fetch(0).start()

                @pl.loop(0, 2 * FF // NB)
                def _(i):
                    @pl.when(i + 1 < 2 * FF // NB)
                    def _():
                        fetch(i + 1).start()

                    fetch(i).wait()
                    j = lax.rem(i, 2)
                    block(T[z, 0, :, c].reshape(TOK, D), T[z, 1, :, c].reshape(TOK, D),
                          wb[j, 0], wb[j, 1], yacc)

            pl.when(e == elast)(epilogue)

        @pl.when((src >= 0) & (src <= 3))
        def _():
            @pl.loop(0, NH)
            def _(h):
                pl.when(h == jnp.where(e == elast, 0, NH // 2))(wpart)
                last = (e == elast) & (h == NH - 1)
                pl.when(last)(flush)

                @pl.when(e > 0)
                def _():
                    with jax.named_scope("tzwait"):
                        tcopy(src, c, h, 0, up).wait_recv()

                    @pl.when((nxt >= 0) & (nxt <= 3))
                    def _():
                        tcopy(src, c, h, 0, (d, 2 * nxt + c)).start()

                    tcopy(src, c, h, 2, partner).start()

                with jax.named_scope("td2dwait"):
                    tcopy(src, o, h, 2, partner).wait_recv()

                @pl.when(last)
                def _():
                    with jax.named_scope("tlast"):
                        pltpu.make_async_copy(T.at[src, :, NH - 1], tl_h, osem.at[4]).start()

                @pl.when(jnp.logical_not(last))
                def _():
                    with jax.named_scope("fside"):
                        block(wo[0], wo[1], T[src, 0, h].reshape(2 * TH, D),
                              T[src, 1, h].reshape(2 * TH, D), wacc)

    dgall = pltpu.make_async_remote_copy(
        src_ref=dgb.at[pl.ds(0, 7)], dst_ref=dgb.at[pl.ds(0, 7)], send_sem=dgs.at[0],
        recv_sem=dgs.at[1], device_id=partner, device_id_type=MESH)
    dgall.wait_recv()
    dgo[...] = jnp.sum(jnp.sum(dgb[...], axis=0), axis=0)
    dgc = pltpu.make_async_copy(dgo, dg_h, osem.at[5])
    dgc.start()

    dgall.wait_send()
    wown(c).wait_send()
    tsent(z, 2)

    @pl.when(z < 3)
    def _():
        wcopy(z, c, d, 0, up).wait_send()
        tsent(z, 0)

    @pl.when(z > 0)
    def _():
        wcopy(z, c, d, 1, down).wait_send()
        tsent(z, 1)

    @pl.loop(1, 7)
    def _(e):
        s = (e + 1) // 2
        sgn = 1 - 2 * (e - 2 * (e // 2))
        src = z + sgn * s
        nxt = z - sgn

        @pl.when((src >= 0) & (src <= 3))
        def _():
            @pl.when((nxt >= 0) & (nxt <= 3))
            def _():
                wcopy(src, c, d, 0, up).wait_send()
                tsent(src, 0)

            wcopy(src, c, 0, 3, partner, 3).wait_send()
            wcopy(src, c, 0, 2, partner, 4).wait_send()
            tsent(src, 2)

    with jax.named_scope("owait"):
        for n in range(2):
            pltpu.make_async_copy(wb.at[1, n], y_h.at[n * NB:(n + 1) * NB, :], osem.at[2 * n]).wait()
            pltpu.make_async_copy(wb.at[0, n], dx_h.at[n * NB:(n + 1) * NB, :], osem.at[2 * n + 1]).wait()
        pltpu.make_async_copy(T.at[z, :, NH - 1], tl_h, osem.at[4]).wait()
        dgc.wait()
        pltpu.make_async_copy(wacc.at[0], wacc.at[0], osem.at[8]).wait()
        pltpu.make_async_copy(wo.at[0], wo.at[0], osem.at[6]).wait()
        pltpu.make_async_copy(wacc.at[1], wacc.at[1], osem.at[7]).wait()


def _finish(tl, w2, *refs):
    p1, p2, w1 = refs[:5], refs[5:10], refs[10:15]
    yv, dxv, dgv, y_h, dx_h, dw1_h, dw2_h, dg_h, o1, o2, osem = refs[15:]
    outs = []

    def out(src, dst):
        cp = pltpu.make_async_copy(src, dst, osem.at[len(outs)])
        cp.start()
        outs.append(cp)

    out(yv, y_h)
    out(dxv, dx_h)
    out(dgv, dg_h)
    xn = tl[0].reshape(2 * TH, D)
    dy = tl[1].reshape(2 * TH, D)
    for r0, r1 in STRIPS:
        r = slice(r0, r1)
        a = _nt(jnp.concatenate([w1[k // 128][...] for k in range(r0, r1, 128)], axis=0), xn)
        g = _nt(w2[r, :], dy)
        h, da = _gelu_pair(a, g)
        q = _nn(h, dy)
        for k in range(r0, r1, 128):
            o2[k:k + 128, :] = p2[k // 128][...] + q[k - r0:k - r0 + 128, :]
        out(o2.at[r, :], dw2_h.at[r, :])
        q = _nn(da, xn)
        for k in range(r0, r1, 128):
            o1[:, k:k + 128] = (p1[k // 128][...] + q[k - r0:k - r0 + 128, :]).T
        out(o1.at[:, r], dw1_h.at[:, r])
    for cp in outs:
        cp.wait()


def solution(mesh):
    rows = P(("data", "tp"), None)
    bf, f32 = jnp.bfloat16, jnp.float32

    def body(X, gamma, W1, W2, dY):
        hbm = pl.BlockSpec(memory_space=pl.ANY)
        vm = pl.BlockSpec(memory_space=pltpu.VMEM)
        sd = jax.ShapeDtypeStruct
        dma = pltpu.SemaphoreType.DMA
        Yp, dXp, *pq = pl.pallas_call(
            _kernel,
            name="mlp_gather",
            out_shape=(sd((TOK, D), bf), sd((TOK, D), bf), *[sd((128, D), f32)] * 10,
                       sd((2, 2, TH, D), bf), sd((4, 2, 2 * FF, D), bf), sd((D,), f32), *[sd((128, D), bf)] * 5),
            in_specs=[hbm] * 5,
            out_specs=[hbm] * 20,
            scratch_shapes=[
                pltpu.VMEM((4, 2, NH, 2, TH, D), bf),
                pltpu.VMEM((2, FF, D), bf),
                pltpu.VMEM((2, 2, NB, D), bf),
                pltpu.VMEM((2, TOK, D), f32),
                pltpu.VMEM((2, FF, D), f32),
                pltpu.VMEM((D,), f32),
                pltpu.VMEM((8, 1, D), f32),
                pltpu.VMEM((8, D), f32),
                pltpu.VMEM((D,), f32),
                dma((4 + 2 * NH + D // NB,)),
                dma((9,)),
                dma((2,)),
                dma((4, 3)),
                dma((4, 2, NH)),
                dma((4, 4)),
                dma((4, 3)),
                dma((2,)),
            ],
            compiler_params=pltpu.CompilerParams(collective_id=0, has_side_effects=True, vmem_limit_bytes=VM1),
        )(*(pltpu.with_memory_space_constraint(v, pltpu.HBM) for v in (X, gamma, W1, W2, dY)))
        return pl.pallas_call(
            _finish,
            name="mlp_finish",
            out_shape=(sd((TOK, D), bf), sd((TOK, D), bf), sd((D, FF), f32), sd((FF, D), f32), sd((D,), f32)),
            in_specs=[vm] * 20,
            out_specs=[hbm] * 5,
            scratch_shapes=[
                pltpu.VMEM((D, FF), f32),
                pltpu.VMEM((FF, D), f32),
                dma((3 + 2 * len(STRIPS),)),
            ],
            compiler_params=pltpu.CompilerParams(vmem_limit_bytes=VM2),
        )(pq[10], W2, *pq[:10], *pq[13:], Yp, dXp, pq[12])

    return jax.shard_map(body, mesh=mesh,
                         in_specs=(rows, P(None), P(None, "tp"), P("tp", None), rows),
                         out_specs=(rows, rows, P("data", "tp"), rows, P("data")),
                         check_vma=False)
```

```python
import functools

import jax
import jax.numpy as jnp
from jax import lax
from jax.experimental import pallas as pl
from jax.experimental.pallas import tpu as pltpu
from jax.sharding import PartitionSpec as P

EPS = 1e-6
D = 1280
TOK = 512
FF = 640
NH = 4
TH = TOK // NH
NB = 256
RT = 64
STRIPS = ((0, 256), (256, 512), (512, 640))
VM1 = 42 * 2**20
VM2 = 20 * 2**20
K0 = 0.7978845608028654
K1 = 0.044715
MESH = pl.DeviceIdType.MESH


def _nt(a, b):
    return lax.dot_general(a, b, (((1,), (1,)), ((), ())), preferred_element_type=jnp.float32)


def _nn(a, b):
    return lax.dot_general(a, b, (((1,), (0,)), ((), ())), preferred_element_type=jnp.float32)


def _tn(a, b):
    return lax.dot_general(a, b, (((0,), (0,)), ((), ())), preferred_element_type=jnp.float32)


def _ln(x):
    mu = jnp.mean(x, axis=-1, keepdims=True)
    xc = x - mu
    var = jnp.mean(xc * xc, axis=-1, keepdims=True)
    rstd = lax.rsqrt(var + EPS)
    return xc * rstd, rstd


def _gelu_pair(a, g):
    a2 = a * a
    t = jnp.tanh(a * (K0 + (K0 * K1) * a2))
    cdf = 0.5 + 0.5 * t
    h = a * cdf
    dg = cdf + h * (1.0 - t) * (K0 + (3.0 * K0 * K1) * a2)
    return h.astype(jnp.bfloat16), (dg * g).astype(jnp.bfloat16)


def _kernel(x_h, g_h, w1_h, w2_h, dy_h, y_h, dx_h, p0, p1, p2, p3, p4, q0, q1, q2, q3, q4, tl_h, W, dg_h, w0_h, w1_o, w2_o, w3_h, w4_h,
            T, wo, wb, yacc, wacc, g_ref, dgb, dgs8, dgo,
            lsem, osem, bsem, tsend, trecv, wsend, wrecv, dgs):
    d = lax.axis_index("data")
    t = lax.axis_index("tp")
    z = t // 2
    c = t - 2 * z
    o = 1 - c
    partner = (d, 2 * z + o)
    up = (d, 2 * z + 2 + c)
    down = (d, 2 * z - 2 + c)
    dxn = lax.rem(d + 2, 4)
    dyn = d + 1 - 2 * lax.rem(d, 2)
    ddg = 3 - d

    def tslot(src, lane, h):
        return T.at[src, :, h, lane]

    def tcopy(src, lane, h, path, dev):
        s = tslot(src, lane, h)
        return pltpu.make_async_remote_copy(
            src_ref=s, dst_ref=s, send_sem=tsend.at[src, path],
            recv_sem=trecv.at[src, lane, h], device_id=dev, device_id_type=MESH)

    def tsent(src, path):
        s = T.at[src, :, :, c]
        pltpu.make_async_remote_copy(
            src_ref=s, dst_ref=s, send_sem=tsend.at[src, path],
            recv_sem=trecv.at[src, c, 0], device_id=partner, device_id_type=MESH).wait_send()

    def wcopy(src, lane, q, path, dev, n=1):
        s = W.at[src, :, pl.ds(pl.multiple_of(lane * FF + q * (FF // 4), 32), n * (FF // 4)), :]
        return pltpu.make_async_remote_copy(
            src_ref=s, dst_ref=s, send_sem=wsend.at[src, path],
            recv_sem=wrecv.at[src, (0, 0, 1, 2, 3)[path]], device_id=dev, device_id_type=MESH)

    def wown(lane):
        return pltpu.make_async_remote_copy(
            src_ref=wo, dst_ref=W.at[z, :, pl.ds(pl.multiple_of(lane * FF, FF), FF), :], send_sem=wsend.at[z, 2],
            recv_sem=wrecv.at[z, 1], device_id=partner, device_id_type=MESH)

    barrier = pltpu.get_barrier_semaphore()

    def greet(dev):
        pl.semaphore_signal(barrier, inc=1, device_id=dev, device_id_type=MESH)

    pl.when(z < 3)(lambda: greet(up))
    pl.when(z > 0)(lambda: greet(down))
    greet(partner)
    for dd in (dxn, dyn):
        greet((dd, t))

    frow = pl.ds(pl.multiple_of(c * FF, FF), FF)
    w1b = [wb.at[i // 4, (i // 2) % 2, :, (i % 2) * FF:(i % 2 + 1) * FF] for i in range(D // NB)]
    l1 = [pltpu.make_async_copy(w1_h.at[i * NB:(i + 1) * NB, :], w1b[i], lsem.at[4 + 2 * NH + i])
          for i in range(D // NB)]
    l2 = pltpu.make_async_copy(w2_h, wo.at[1], lsem.at[1])
    for cp in l1:
        cp.start()
    l2.start()
    l3 = [pltpu.make_async_copy(x_h.at[pl.ds(h * TH, TH), :], T.at[z, 0, h, c], lsem.at[4 + NH + h])
          for h in range(NH)]
    for cp in l3:
        cp.start()
    lg = pltpu.make_async_copy(g_h, g_ref, lsem.at[0])
    lg.start()
    l4 = [pltpu.make_async_copy(dy_h.at[pl.ds(h * TH, TH), :], T.at[z, 1, h, c], lsem.at[3 + h])
          for h in range(NH)]
    for cp in l4:
        cp.start()
    pl.semaphore_wait(barrier, 3 + (z > 0).astype(jnp.int32) + (z < 3).astype(jnp.int32))

    def whalf(mat, path, dev):
        q = pl.ds(pl.multiple_of(d * (FF // 4), 32), FF // 4)
        return pltpu.make_async_remote_copy(
            src_ref=w2_h.at[q, :] if mat else wo.at[0, q, :],
            dst_ref=W.at[z, mat, pl.ds(pl.multiple_of(c * FF + d * (FF // 4), 32), FF // 4), :], send_sem=wsend.at[z, path],
            recv_sem=wrecv.at[z, 0], device_id=dev, device_id_type=MESH)

    @pl.when(z < 3)
    def _():
        whalf(1, 0, up).start()

    @pl.when(z > 0)
    def _():
        whalf(1, 1, down).start()

    for i in range(D // NB):
        l1[i].wait()
        wo[0, :, i * NB:(i + 1) * NB] = w1b[i][...].T

    l2.wait()
    lg.wait()
    for cp in l3:
        cp.wait()

    @pl.loop(0, TOK // RT)
    def _(i):
        r = pl.ds(pl.multiple_of(i * RT, RT), RT)
        h = i // (TH // RT)
        rr = pl.ds(pl.multiple_of((i - h * (TH // RT)) * RT, RT), RT)
        x = T[z, 0, h, c, rr, :].astype(jnp.float32)
        xh, _ = _ln(x)
        T[z, 0, h, c, rr, :] = (xh * g_ref[...].reshape(1, D)).astype(jnp.bfloat16)
        yacc[1, r, :] = x
        yacc[0, r, :] = jnp.zeros((RT, D), jnp.float32)

    @pl.when(z < 3)
    def _():
        whalf(0, 0, up).start()

    @pl.when(z > 0)
    def _():
        whalf(0, 1, down).start()

    wown(c).start()
    lo = pltpu.make_async_copy(wo, W.at[z, :, frow, :], lsem.at[3 + NH])
    lo.start()

    @pl.loop(0, FF // RT)
    def _(i):
        r = pl.ds(pl.multiple_of(i * RT, RT), RT)
        wacc[0, r, :] = jnp.zeros((RT, D), jnp.float32)
        wacc[1, r, :] = jnp.zeros((RT, D), jnp.float32)

    for cp in l4:
        cp.wait()

    def town(h0, h1):
        @pl.when(z < 3)
        def _():
            for h in range(h0, h1):
                tcopy(z, c, h, 0, up).start()

        @pl.when(z > 0)
        def _():
            for h in range(h0, h1):
                tcopy(z, c, h, 1, down).start()

    town(0, NH // 2)
    for h in range(NH):
        tcopy(z, c, h, 2, partner).start()

    def wstep(s):
        for sgn in (-1, 1):
            src = z + sgn * s

            @pl.when((src >= 0) & (src <= 3))
            def _():
                with jax.named_scope("wzwait"):
                    wcopy(src, c, d, 0, up).wait_recv()

                @pl.when((z - sgn >= 0) & (z - sgn <= 3))
                def _():
                    wcopy(src, c, d, 0, (d, 2 * (z - sgn) + c)).start()

                for dd in (dxn, dyn):
                    wcopy(src, c, d, 3, (dd, t)).start()

                @pl.when(s > 1)
                def _():
                    wcopy(src, c, d, 4, (ddg, t)).start()

                wcopy(src, c, d, 2, partner).start()

    def block(l1, l2, r1, r2, acc):
        a = _nt(l1, r1)
        g = _nt(l2, r2)
        h, da = _gelu_pair(a, g)
        acc[1, :, :] += _nn(h, r2)
        acc[0, :, :] += _nn(da, r1)

    elast = jnp.where(z == 0, 6, jnp.where(z == 3, 5, jnp.where(z == 1, 4, 3)))

    @pl.loop(0, 7)
    def _(e):
        s = (e + 1) // 2
        sgn = 1 - 2 * (e - 2 * (e // 2))
        src = z + sgn * s
        nxt = z - sgn

        @pl.when((e == 0) | (e == 1) | (e == 3))
        def _():
            wstep(jnp.where(e == 0, 1, jnp.where(e == 1, 2, 3)))

        @pl.when(e == 0)
        def _():
            town(NH // 2, NH)

        def wside(src):
            with jax.named_scope("wxywait"):
                wcopy(src, c, 0, 3, partner, 2).wait_recv()
                for dd in (dxn, dyn):
                    wcopy(src, c, dd, 2, partner).start()

        def xcopy(n):
            return pltpu.make_async_copy(x_h.at[n * NB:(n + 1) * NB, :], wb.at[0, n], bsem.at[n])

        def epilogue():
            for n in range(2):
                xcopy(n).start()
            for n in range(2):
                xcopy(n).wait()
            dgs8[...] = jnp.zeros((8, D), jnp.float32)

            @pl.loop(0, TOK // RT)
            def _(i):
                r = pl.ds(pl.multiple_of(i * RT, RT), RT)
                n = i // (NB // RT)
                wr = pl.ds(pl.multiple_of((i - n * (NB // RT)) * RT, RT), RT)
                x = wb[0, n, wr, :].astype(jnp.float32)
                xh, rstd = _ln(x)
                dxn_ = yacc[0, r, :]
                p = dxn_ * xh
                dgs8[...] += jnp.sum(p.reshape(RT // 8, 8, D), axis=0)
                dxh = dxn_ * g_ref[...].reshape(1, D)
                m1 = jnp.mean(dxh, axis=-1, keepdims=True)
                m2 = jnp.mean(dxh * xh, axis=-1, keepdims=True)
                h = i // (TH // RT)
                rr = pl.ds(pl.multiple_of((i - h * (TH // RT)) * RT, RT), RT)
                dyv = T[z, 1, h, c, rr, :].astype(jnp.float32)
                wb[0, n, wr, :] = (dyv + rstd * (dxh - m1 - xh * m2)).astype(jnp.bfloat16)
                wb[1, n, wr, :] = yacc[1, r, :].astype(jnp.bfloat16)

            dgb[t] = jnp.sum(dgs8[...], axis=0, keepdims=True)
            for n in range(2):
                pltpu.make_async_copy(wb.at[1, n], y_h.at[n * NB:(n + 1) * NB, :], osem.at[2 * n]).start()
                pltpu.make_async_copy(wb.at[0, n], dx_h.at[n * NB:(n + 1) * NB, :], osem.at[2 * n + 1]).start()
            for k in range(1, 8):
                pltpu.make_async_remote_copy(
                    src_ref=dgb.at[t], dst_ref=dgb.at[t], send_sem=dgs.at[0],
                    recv_sem=dgs.at[1], device_id=(d, lax.rem(t + k, 8)),
                    device_id_type=MESH).start()

        def flush():
            with jax.named_scope("flush"):
                for i in range(5):
                    pltpu.make_async_copy(wacc.at[1, i * 128:(i + 1) * 128, :], (q0, q1, q2, q3, q4)[i], osem.at[7]).start()
                for i in range(5):
                    pltpu.make_async_copy(wacc.at[0, i * 128:(i + 1) * 128, :], (p0, p1, p2, p3, p4)[i], osem.at[8]).start()
                for i in range(5):
                    pltpu.make_async_copy(wo.at[0, i * 128:(i + 1) * 128, :], (w0_h, w1_o, w2_o, w3_h, w4_h)[i],
                                          osem.at[6]).start()

        def wpart():
            @pl.when(e == 0)
            def _():
                wown(o).wait_recv()
                lo.wait()

            @pl.when(e > 0)
            def _():
                pl.when(s > 1)(lambda: wside(src))
                with jax.named_scope("wdgwait"):
                    wcopy(src, c, 0, 4, partner).wait_recv()
                    wcopy(src, c, ddg, 2, partner).start()
                with jax.named_scope("wd2dwait"):
                    wcopy(src, o, 0, 2, partner, 4).wait_recv()

            with jax.named_scope("tokside"):
                def fetch(i):
                    j = lax.rem(i, 2)
                    rr = pl.ds(pl.multiple_of(i * NB, NB), NB)
                    return pltpu.make_async_copy(W.at[src, :, rr, :], wb.at[j], bsem.at[j])

                fetch(0).start()

                @pl.loop(0, 2 * FF // NB)
                def _(i):
                    @pl.when(i + 1 < 2 * FF // NB)
                    def _():
                        fetch(i + 1).start()

                    fetch(i).wait()
                    j = lax.rem(i, 2)
                    block(T[z, 0, :, c].reshape(TOK, D), T[z, 1, :, c].reshape(TOK, D),
                          wb[j, 0], wb[j, 1], yacc)

            pl.when(e == elast)(epilogue)

        @pl.when((src >= 0) & (src <= 3))
        def _():
            @pl.loop(0, NH)
            def _(h):
                pl.when(h == jnp.where(e == elast, 0, NH // 2))(wpart)
                last = (e == elast) & (h == NH - 1)
                pl.when(last)(flush)

                @pl.when(e > 0)
                def _():
                    with jax.named_scope("tzwait"):
                        tcopy(src, c, h, 0, up).wait_recv()

                    @pl.when((nxt >= 0) & (nxt <= 3))
                    def _():
                        tcopy(src, c, h, 0, (d, 2 * nxt + c)).start()

                    tcopy(src, c, h, 2, partner).start()

                with jax.named_scope("td2dwait"):
                    tcopy(src, o, h, 2, partner).wait_recv()

                @pl.when(last)
                def _():
                    with jax.named_scope("tlast"):
                        pltpu.make_async_copy(T.at[src, :, NH - 1], tl_h, osem.at[4]).start()

                @pl.when(jnp.logical_not(last))
                def _():
                    with jax.named_scope("fside"):
                        block(wo[0], wo[1], T[src, 0, h].reshape(2 * TH, D),
                              T[src, 1, h].reshape(2 * TH, D), wacc)

        @pl.when(e == 0)
        def _():
            for sg in (-1, 1):
                near = z + sg

                @pl.when((near >= 0) & (near <= 3))
                def _():
                    wside(near)
                    wcopy(near, c, d, 4, (ddg, t)).start()

    dgall = pltpu.make_async_remote_copy(
        src_ref=dgb.at[pl.ds(0, 7)], dst_ref=dgb.at[pl.ds(0, 7)], send_sem=dgs.at[0],
        recv_sem=dgs.at[1], device_id=partner, device_id_type=MESH)
    dgall.wait_recv()
    dgo[...] = jnp.sum(jnp.sum(dgb[...], axis=0), axis=0)
    dgc = pltpu.make_async_copy(dgo, dg_h, osem.at[5])
    dgc.start()

    dgall.wait_send()
    wown(c).wait_send()
    tsent(z, 2)

    @pl.when(z < 3)
    def _():
        wcopy(z, c, d, 0, up).wait_send()
        tsent(z, 0)

    @pl.when(z > 0)
    def _():
        wcopy(z, c, d, 1, down).wait_send()
        tsent(z, 1)

    @pl.loop(1, 7)
    def _(e):
        s = (e + 1) // 2
        sgn = 1 - 2 * (e - 2 * (e // 2))
        src = z + sgn * s
        nxt = z - sgn

        @pl.when((src >= 0) & (src <= 3))
        def _():
            @pl.when((nxt >= 0) & (nxt <= 3))
            def _():
                wcopy(src, c, d, 0, up).wait_send()
                tsent(src, 0)

            wcopy(src, c, 0, 3, partner, 2).wait_send()
            wcopy(src, c, 0, 4, partner).wait_send()
            wcopy(src, c, 0, 2, partner, 4).wait_send()
            tsent(src, 2)

    with jax.named_scope("owait"):
        for n in range(2):
            pltpu.make_async_copy(wb.at[1, n], y_h.at[n * NB:(n + 1) * NB, :], osem.at[2 * n]).wait()
            pltpu.make_async_copy(wb.at[0, n], dx_h.at[n * NB:(n + 1) * NB, :], osem.at[2 * n + 1]).wait()
        pltpu.make_async_copy(T.at[z, :, NH - 1], tl_h, osem.at[4]).wait()
        dgc.wait()
        pltpu.make_async_copy(wacc.at[0], wacc.at[0], osem.at[8]).wait()
        pltpu.make_async_copy(wo.at[0], wo.at[0], osem.at[6]).wait()
        pltpu.make_async_copy(wacc.at[1], wacc.at[1], osem.at[7]).wait()


def _finish(tl, w2, *refs):
    p1, p2, w1 = refs[:5], refs[5:10], refs[10:15]
    yv, dxv, dgv, y_h, dx_h, dw1_h, dw2_h, dg_h, o1, o2, osem = refs[15:]
    outs = []

    def out(src, dst):
        cp = pltpu.make_async_copy(src, dst, osem.at[len(outs)])
        cp.start()
        outs.append(cp)

    out(yv, y_h)
    out(dxv, dx_h)
    out(dgv, dg_h)
    xn = tl[0].reshape(2 * TH, D)
    dy = tl[1].reshape(2 * TH, D)
    for r0, r1 in STRIPS:
        r = slice(r0, r1)
        a = _nt(jnp.concatenate([w1[k // 128][...] for k in range(r0, r1, 128)], axis=0), xn)
        g = _nt(w2[r, :], dy)
        h, da = _gelu_pair(a, g)
        q = _nn(h, dy)
        for k in range(r0, r1, 128):
            o2[k:k + 128, :] = p2[k // 128][...] + q[k - r0:k - r0 + 128, :]
        out(o2.at[r, :], dw2_h.at[r, :])
        q = _nn(da, xn)
        for k in range(r0, r1, 128):
            o1[:, k:k + 128] = (p1[k // 128][...] + q[k - r0:k - r0 + 128, :]).T
        out(o1.at[:, r], dw1_h.at[:, r])
    for cp in outs:
        cp.wait()


def solution(mesh):
    rows = P(("data", "tp"), None)
    bf, f32 = jnp.bfloat16, jnp.float32

    def body(X, gamma, W1, W2, dY):
        hbm = pl.BlockSpec(memory_space=pl.ANY)
        vm = pl.BlockSpec(memory_space=pltpu.VMEM)
        sd = jax.ShapeDtypeStruct
        dma = pltpu.SemaphoreType.DMA
        Yp, dXp, *pq = pl.pallas_call(
            _kernel,
            name="mlp_gather",
            out_shape=(sd((TOK, D), bf), sd((TOK, D), bf), *[sd((128, D), f32)] * 10,
                       sd((2, 2, TH, D), bf), sd((4, 2, 2 * FF, D), bf), sd((D,), f32), *[sd((128, D), bf)] * 5),
            in_specs=[hbm] * 5,
            out_specs=[hbm] * 20,
            scratch_shapes=[
                pltpu.VMEM((4, 2, NH, 2, TH, D), bf),
                pltpu.VMEM((2, FF, D), bf),
                pltpu.VMEM((2, 2, NB, D), bf),
                pltpu.VMEM((2, TOK, D), f32),
                pltpu.VMEM((2, FF, D), f32),
                pltpu.VMEM((D,), f32),
                pltpu.VMEM((8, 1, D), f32),
                pltpu.VMEM((8, D), f32),
                pltpu.VMEM((D,), f32),
                dma((4 + 2 * NH + D // NB,)),
                dma((9,)),
                dma((2,)),
                dma((4, 3)),
                dma((4, 2, NH)),
                dma((4, 5)),
                dma((4, 4)),
                dma((2,)),
            ],
            compiler_params=pltpu.CompilerParams(collective_id=0, has_side_effects=True, vmem_limit_bytes=VM1),
        )(*(pltpu.with_memory_space_constraint(v, pltpu.HBM) for v in (X, gamma, W1, W2, dY)))
        return pl.pallas_call(
            _finish,
            name="mlp_finish",
            out_shape=(sd((TOK, D), bf), sd((TOK, D), bf), sd((D, FF), f32), sd((FF, D), f32), sd((D,), f32)),
            in_specs=[vm] * 20,
            out_specs=[hbm] * 5,
            scratch_shapes=[
                pltpu.VMEM((D, FF), f32),
                pltpu.VMEM((FF, D), f32),
                dma((3 + 2 * len(STRIPS),)),
            ],
            compiler_params=pltpu.CompilerParams(vmem_limit_bytes=VM2),
        )(pq[10], W2, *pq[:10], *pq[13:], Yp, dXp, pq[12])

    return jax.shard_map(body, mesh=mesh,
                         in_specs=(rows, P(None), P(None, "tp"), P("tp", None), rows),
                         out_specs=(rows, rows, P("data", "tp"), rows, P("data")),
                         check_vma=False)
```

```python
import functools

import jax
import jax.numpy as jnp
from jax import lax
from jax.experimental import pallas as pl
from jax.experimental.pallas import tpu as pltpu
from jax.sharding import PartitionSpec as P

EPS = 1e-6
D = 1280
TOK = 512
FF = 640
NH = 4
TH = TOK // NH
NB = 256
RT = 64
STRIPS = ((0, 256), (256, 512), (512, 640))
VM1 = 42 * 2**20
VM2 = 20 * 2**20
K0 = 0.7978845608028654
K1 = 0.044715
MESH = pl.DeviceIdType.MESH


def _nt(a, b):
    return lax.dot_general(a, b, (((1,), (1,)), ((), ())), preferred_element_type=jnp.float32)


def _nn(a, b):
    return lax.dot_general(a, b, (((1,), (0,)), ((), ())), preferred_element_type=jnp.float32)


def _tn(a, b):
    return lax.dot_general(a, b, (((0,), (0,)), ((), ())), preferred_element_type=jnp.float32)


def _ln(x):
    mu = jnp.mean(x, axis=-1, keepdims=True)
    xc = x - mu
    var = jnp.mean(xc * xc, axis=-1, keepdims=True)
    rstd = lax.rsqrt(var + EPS)
    return xc * rstd, rstd


def _gelu_pair(a, g):
    a2 = a * a
    t = jnp.tanh(a * (K0 + (K0 * K1) * a2))
    cdf = 0.5 + 0.5 * t
    h = a * cdf
    dg = cdf + h * (1.0 - t) * (K0 + (3.0 * K0 * K1) * a2)
    return h.astype(jnp.bfloat16), (dg * g).astype(jnp.bfloat16)


def _kernel(x_h, g_h, w1_h, w2_h, dy_h, y_h, dx_h, p0, p1, p2, p3, p4, q0, q1, q2, q3, q4, tl_h, W, dg_h, w0_h, w1_o, w2_o, w3_h, w4_h,
            T, wo, wb, yacc, wacc, g_ref, dgb, dgs8, dgo,
            lsem, osem, bsem, tsend, trecv, wsend, wrecv, dgs):
    d = lax.axis_index("data")
    t = lax.axis_index("tp")
    z = t // 2
    c = t - 2 * z
    o = 1 - c
    partner = (d, 2 * z + o)
    up = (d, 2 * z + 2 + c)
    down = (d, 2 * z - 2 + c)
    dxn = lax.rem(d + 2, 4)
    dyn = d + 1 - 2 * lax.rem(d, 2)
    ddg = 3 - d

    def tslot(src, lane, h):
        return T.at[src, :, h, lane]

    def tcopy(src, lane, h, path, dev):
        s = tslot(src, lane, h)
        return pltpu.make_async_remote_copy(
            src_ref=s, dst_ref=s, send_sem=tsend.at[src, path],
            recv_sem=trecv.at[src, lane, h], device_id=dev, device_id_type=MESH)

    def tsent(src, path):
        s = T.at[src, :, :, c]
        pltpu.make_async_remote_copy(
            src_ref=s, dst_ref=s, send_sem=tsend.at[src, path],
            recv_sem=trecv.at[src, c, 0], device_id=partner, device_id_type=MESH).wait_send()

    def wcopy(src, lane, q, path, dev, n=1):
        s = W.at[src, :, pl.ds(pl.multiple_of(lane * FF + q * (FF // 4), 32), n * (FF // 4)), :]
        return pltpu.make_async_remote_copy(
            src_ref=s, dst_ref=s, send_sem=wsend.at[src, path],
            recv_sem=wrecv.at[src, (0, 0, 1, 2, 3)[path]], device_id=dev, device_id_type=MESH)

    def wown(lane):
        return pltpu.make_async_remote_copy(
            src_ref=wo, dst_ref=W.at[z, :, pl.ds(pl.multiple_of(lane * FF, FF), FF), :], send_sem=wsend.at[z, 2],
            recv_sem=wrecv.at[z, 1], device_id=partner, device_id_type=MESH)

    barrier = pltpu.get_barrier_semaphore()

    def greet(dev):
        pl.semaphore_signal(barrier, inc=1, device_id=dev, device_id_type=MESH)

    pl.when(z < 3)(lambda: greet(up))
    pl.when(z > 0)(lambda: greet(down))
    greet(partner)
    for dd in (dxn, dyn):
        greet((dd, t))

    frow = pl.ds(pl.multiple_of(c * FF, FF), FF)
    w1b = [wb.at[i // 4, (i // 2) % 2, :, (i % 2) * FF:(i % 2 + 1) * FF] for i in range(D // NB)]
    l1 = [pltpu.make_async_copy(w1_h.at[i * NB:(i + 1) * NB, :], w1b[i], lsem.at[2])
          for i in range(D // NB)]
    l2 = pltpu.make_async_copy(w2_h, wo.at[1], lsem.at[1])
    for cp in l1:
        cp.start()
    l2.start()
    l3 = [pltpu.make_async_copy(x_h.at[pl.ds(h * TH, TH), :], T.at[z, 0, h, c], lsem.at[3])
          for h in range(NH)]
    for cp in l3:
        cp.start()
    lg = pltpu.make_async_copy(g_h, g_ref, lsem.at[0])
    lg.start()
    l4 = [pltpu.make_async_copy(dy_h.at[pl.ds(h * TH, TH), :], T.at[z, 1, h, c], lsem.at[4])
          for h in range(NH)]
    for cp in l4:
        cp.start()
    pl.semaphore_wait(barrier, 3 + (z > 0).astype(jnp.int32) + (z < 3).astype(jnp.int32))

    def whalf(mat, path, dev):
        q = pl.ds(pl.multiple_of(d * (FF // 4), 32), FF // 4)
        return pltpu.make_async_remote_copy(
            src_ref=w2_h.at[q, :] if mat else wo.at[0, q, :],
            dst_ref=W.at[z, mat, pl.ds(pl.multiple_of(c * FF + d * (FF // 4), 32), FF // 4), :], send_sem=wsend.at[z, path],
            recv_sem=wrecv.at[z, 0], device_id=dev, device_id_type=MESH)

    @pl.when(z < 3)
    def _():
        whalf(1, 0, up).start()

    @pl.when(z > 0)
    def _():
        whalf(1, 1, down).start()

    pltpu.make_async_copy(wo.at[0], wo.at[0], lsem.at[2]).wait()
    for i in range(D // NB):
        wo[0, :, i * NB:(i + 1) * NB] = w1b[i][...].T

    l2.wait()
    lg.wait()
    pltpu.make_async_copy(T.at[z, 0, :, c], T.at[z, 0, :, c], lsem.at[3]).wait()

    @pl.loop(0, TOK // RT)
    def _(i):
        r = pl.ds(pl.multiple_of(i * RT, RT), RT)
        h = i // (TH // RT)
        rr = pl.ds(pl.multiple_of((i - h * (TH // RT)) * RT, RT), RT)
        x = T[z, 0, h, c, rr, :].astype(jnp.float32)
        xh, _ = _ln(x)
        T[z, 0, h, c, rr, :] = (xh * g_ref[...].reshape(1, D)).astype(jnp.bfloat16)
        yacc[1, r, :] = x
        yacc[0, r, :] = jnp.zeros((RT, D), jnp.float32)

    @pl.when(z < 3)
    def _():
        whalf(0, 0, up).start()

    @pl.when(z > 0)
    def _():
        whalf(0, 1, down).start()

    wown(c).start()
    lo = pltpu.make_async_copy(wo, W.at[z, :, frow, :], lsem.at[5])
    lo.start()

    @pl.loop(0, FF // RT)
    def _(i):
        r = pl.ds(pl.multiple_of(i * RT, RT), RT)
        wacc[0, r, :] = jnp.zeros((RT, D), jnp.float32)
        wacc[1, r, :] = jnp.zeros((RT, D), jnp.float32)

    pltpu.make_async_copy(T.at[z, 1, :, c], T.at[z, 1, :, c], lsem.at[4]).wait()

    def town(h0, h1):
        @pl.when(z < 3)
        def _():
            for h in range(h0, h1):
                tcopy(z, c, h, 0, up).start()

        @pl.when(z > 0)
        def _():
            for h in range(h0, h1):
                tcopy(z, c, h, 1, down).start()

    town(0, NH // 2)
    for h in range(NH):
        tcopy(z, c, h, 2, partner).start()

    def wstep(s):
        for sgn in (-1, 1):
            src = z + sgn * s

            @pl.when((src >= 0) & (src <= 3))
            def _():
                with jax.named_scope("wzwait"):
                    wcopy(src, c, d, 0, up).wait_recv()

                @pl.when((z - sgn >= 0) & (z - sgn <= 3))
                def _():
                    wcopy(src, c, d, 0, (d, 2 * (z - sgn) + c)).start()

                for dd in (dxn, dyn):
                    wcopy(src, c, d, 3, (dd, t)).start()

                @pl.when(s > 1)
                def _():
                    wcopy(src, c, d, 4, (ddg, t)).start()

                wcopy(src, c, d, 2, partner).start()

    def block(l1, l2, r1, r2, acc):
        a = _nt(l1, r1)
        g = _nt(l2, r2)
        h, da = _gelu_pair(a, g)
        acc[1, :, :] += _nn(h, r2)
        acc[0, :, :] += _nn(da, r1)

    elast = jnp.where(z == 0, 6, jnp.where(z == 3, 5, jnp.where(z == 1, 4, 3)))

    @pl.loop(0, 7)
    def _(e):
        s = (e + 1) // 2
        sgn = 1 - 2 * (e - 2 * (e // 2))
        src = z + sgn * s
        nxt = z - sgn

        @pl.when((e == 0) | (e == 1) | (e == 3))
        def _():
            wstep(jnp.where(e == 0, 1, jnp.where(e == 1, 2, 3)))

        @pl.when(e == 0)
        def _():
            town(NH // 2, NH)

        def wside(src):
            with jax.named_scope("wxywait"):
                wcopy(src, c, 0, 3, partner, 2).wait_recv()
                for dd in (dxn, dyn):
                    wcopy(src, c, dd, 2, partner).start()

        def dgpair(lane):
            return pltpu.make_async_remote_copy(
                src_ref=dgb.at[4 + lane], dst_ref=dgb.at[4 + lane], send_sem=dgs.at[2],
                recv_sem=dgs.at[3], device_id=partner, device_id_type=MESH)

        def xcopy(n):
            return pltpu.make_async_copy(x_h.at[n * NB:(n + 1) * NB, :], wb.at[0, n], bsem.at[n])

        def epilogue():
            for n in range(2):
                xcopy(n).start()
            for n in range(2):
                xcopy(n).wait()
            dgs8[...] = jnp.zeros((8, D), jnp.float32)

            @pl.loop(0, TOK // RT)
            def _(i):
                r = pl.ds(pl.multiple_of(i * RT, RT), RT)
                n = i // (NB // RT)
                wr = pl.ds(pl.multiple_of((i - n * (NB // RT)) * RT, RT), RT)
                x = wb[0, n, wr, :].astype(jnp.float32)
                xh, rstd = _ln(x)
                dxn_ = yacc[0, r, :]
                p = dxn_ * xh
                dgs8[...] += jnp.sum(p.reshape(RT // 8, 8, D), axis=0)
                dxh = dxn_ * g_ref[...].reshape(1, D)
                m1 = jnp.mean(dxh, axis=-1, keepdims=True)
                m2 = jnp.mean(dxh * xh, axis=-1, keepdims=True)
                h = i // (TH // RT)
                rr = pl.ds(pl.multiple_of((i - h * (TH // RT)) * RT, RT), RT)
                dyv = T[z, 1, h, c, rr, :].astype(jnp.float32)
                wb[0, n, wr, :] = (dyv + rstd * (dxh - m1 - xh * m2)).astype(jnp.bfloat16)
                wb[1, n, wr, :] = yacc[1, r, :].astype(jnp.bfloat16)

            dgb[4 + c] = jnp.sum(dgs8[...], axis=0, keepdims=True)
            for n in range(2):
                pltpu.make_async_copy(wb.at[1, n], y_h.at[n * NB:(n + 1) * NB, :], osem.at[2 * n]).start()
            dgpair(c).start()
            dgpair(o).wait_recv()
            dgb[z] = dgb[4] + dgb[5]
            for n in range(2):
                pltpu.make_async_copy(wb.at[0, n], dx_h.at[n * NB:(n + 1) * NB, :], osem.at[2 * n + 1]).start()
            for k in range(1, 4):
                pltpu.make_async_remote_copy(
                    src_ref=dgb.at[z], dst_ref=dgb.at[z], send_sem=dgs.at[0],
                    recv_sem=dgs.at[1], device_id=(d, 2 * lax.rem(z + k, 4) + c),
                    device_id_type=MESH).start()

        def flush():
            with jax.named_scope("flush"):
                for i in range(5):
                    pltpu.make_async_copy(wacc.at[1, i * 128:(i + 1) * 128, :], (q0, q1, q2, q3, q4)[i], osem.at[7]).start()
                for i in range(5):
                    pltpu.make_async_copy(wacc.at[0, i * 128:(i + 1) * 128, :], (p0, p1, p2, p3, p4)[i], osem.at[8]).start()
                for i in range(5):
                    pltpu.make_async_copy(wo.at[0, i * 128:(i + 1) * 128, :], (w0_h, w1_o, w2_o, w3_h, w4_h)[i],
                                          osem.at[6]).start()

        def wpart():
            @pl.when(e == 0)
            def _():
                wown(o).wait_recv()
                lo.wait()

            @pl.when(e > 0)
            def _():
                pl.when(s > 1)(lambda: wside(src))
                with jax.named_scope("wdgwait"):
                    wcopy(src, c, 0, 4, partner).wait_recv()
                    wcopy(src, c, ddg, 2, partner).start()
                with jax.named_scope("wd2dwait"):
                    wcopy(src, o, 0, 2, partner, 4).wait_recv()

            with jax.named_scope("tokside"):
                def fetch(i):
                    j = lax.rem(i, 2)
                    rr = pl.ds(pl.multiple_of(i * NB, NB), NB)
                    return pltpu.make_async_copy(W.at[src, :, rr, :], wb.at[j], bsem.at[j])

                fetch(0).start()

                @pl.loop(0, 2 * FF // NB)
                def _(i):
                    @pl.when(i + 1 < 2 * FF // NB)
                    def _():
                        fetch(i + 1).start()

                    fetch(i).wait()
                    j = lax.rem(i, 2)
                    block(T[z, 0, :, c].reshape(TOK, D), T[z, 1, :, c].reshape(TOK, D),
                          wb[j, 0], wb[j, 1], yacc)

            pl.when(e == elast)(epilogue)

        @pl.when((src >= 0) & (src <= 3))
        def _():
            @pl.loop(0, NH)
            def _(h):
                pl.when(h == jnp.where(e == elast, 0, NH // 2))(wpart)
                last = (e == elast) & (h == NH - 1)
                pl.when(last)(flush)

                @pl.when(e > 0)
                def _():
                    with jax.named_scope("tzwait"):
                        tcopy(src, c, h, 0, up).wait_recv()

                    @pl.when((nxt >= 0) & (nxt <= 3))
                    def _():
                        tcopy(src, c, h, 0, (d, 2 * nxt + c)).start()

                    tcopy(src, c, h, 2, partner).start()

                with jax.named_scope("td2dwait"):
                    tcopy(src, o, h, 2, partner).wait_recv()

                @pl.when(last)
                def _():
                    with jax.named_scope("tlast"):
                        pltpu.make_async_copy(T.at[src, :, NH - 1], tl_h, osem.at[4]).start()

                @pl.when(jnp.logical_not(last))
                def _():
                    with jax.named_scope("fside"):
                        block(wo[0], wo[1], T[src, 0, h].reshape(2 * TH, D),
                              T[src, 1, h].reshape(2 * TH, D), wacc)

        @pl.when(e == 0)
        def _():
            for sg in (-1, 1):
                near = z + sg

                @pl.when((near >= 0) & (near <= 3))
                def _():
                    wside(near)
                    wcopy(near, c, d, 4, (ddg, t)).start()

    dgall = pltpu.make_async_remote_copy(
        src_ref=dgb.at[pl.ds(0, 3)], dst_ref=dgb.at[pl.ds(0, 3)], send_sem=dgs.at[0],
        recv_sem=dgs.at[1], device_id=partner, device_id_type=MESH)
    dgall.wait_recv()
    dgo[...] = jnp.sum(jnp.sum(dgb[0:4], axis=0), axis=0)
    dgc = pltpu.make_async_copy(dgo, dg_h, osem.at[5])
    dgc.start()

    dgall.wait_send()
    pltpu.make_async_remote_copy(
        src_ref=dgb.at[4], dst_ref=dgb.at[4], send_sem=dgs.at[2],
        recv_sem=dgs.at[3], device_id=partner, device_id_type=MESH).wait_send()
    wown(c).wait_send()
    tsent(z, 2)

    @pl.when(z < 3)
    def _():
        wcopy(z, c, d, 0, up).wait_send()
        tsent(z, 0)

    @pl.when(z > 0)
    def _():
        wcopy(z, c, d, 1, down).wait_send()
        tsent(z, 1)

    @pl.loop(1, 7)
    def _(e):
        s = (e + 1) // 2
        sgn = 1 - 2 * (e - 2 * (e // 2))
        src = z + sgn * s
        nxt = z - sgn

        @pl.when((src >= 0) & (src <= 3))
        def _():
            @pl.when((nxt >= 0) & (nxt <= 3))
            def _():
                wcopy(src, c, d, 0, up).wait_send()
                tsent(src, 0)

            wcopy(src, c, 0, 3, partner, 2).wait_send()
            wcopy(src, c, 0, 4, partner).wait_send()
            wcopy(src, c, 0, 2, partner, 4).wait_send()
            tsent(src, 2)

    with jax.named_scope("owait"):
        for n in range(2):
            pltpu.make_async_copy(wb.at[1, n], y_h.at[n * NB:(n + 1) * NB, :], osem.at[2 * n]).wait()
            pltpu.make_async_copy(wb.at[0, n], dx_h.at[n * NB:(n + 1) * NB, :], osem.at[2 * n + 1]).wait()
        pltpu.make_async_copy(T.at[z, :, NH - 1], tl_h, osem.at[4]).wait()
        dgc.wait()
        pltpu.make_async_copy(wacc.at[0], wacc.at[0], osem.at[8]).wait()
        pltpu.make_async_copy(wo.at[0], wo.at[0], osem.at[6]).wait()
        pltpu.make_async_copy(wacc.at[1], wacc.at[1], osem.at[7]).wait()


def _finish(tl, w2, *refs):
    p1, p2, w1 = refs[:5], refs[5:10], refs[10:15]
    yv, dxv, dgv, y_h, dx_h, dw1_h, dw2_h, dg_h, o1, o2, osem = refs[15:]
    outs = []

    def out(src, dst):
        cp = pltpu.make_async_copy(src, dst, osem.at[len(outs)])
        cp.start()
        outs.append(cp)

    out(yv, y_h)
    out(dxv, dx_h)
    out(dgv, dg_h)
    xn = tl[0].reshape(2 * TH, D)
    dy = tl[1].reshape(2 * TH, D)
    for r0, r1 in STRIPS:
        r = slice(r0, r1)
        a = _nt(jnp.concatenate([w1[k // 128][...] for k in range(r0, r1, 128)], axis=0), xn)
        g = _nt(w2[r, :], dy)
        h, da = _gelu_pair(a, g)
        q = _nn(h, dy)
        for k in range(r0, r1, 128):
            o2[k:k + 128, :] = p2[k // 128][...] + q[k - r0:k - r0 + 128, :]
        out(o2.at[r, :], dw2_h.at[r, :])
        q = _nn(da, xn)
        for k in range(r0, r1, 128):
            o1[:, k:k + 128] = (p1[k // 128][...] + q[k - r0:k - r0 + 128, :]).T
        out(o1.at[:, r], dw1_h.at[:, r])
    for cp in outs:
        cp.wait()


def solution(mesh):
    rows = P(("data", "tp"), None)
    bf, f32 = jnp.bfloat16, jnp.float32

    def body(X, gamma, W1, W2, dY):
        hbm = pl.BlockSpec(memory_space=pl.ANY)
        vm = pl.BlockSpec(memory_space=pltpu.VMEM)
        sd = jax.ShapeDtypeStruct
        dma = pltpu.SemaphoreType.DMA
        Yp, dXp, *pq = pl.pallas_call(
            _kernel,
            name="mlp_gather",
            out_shape=(sd((TOK, D), bf), sd((TOK, D), bf), *[sd((128, D), f32)] * 10,
                       sd((2, 2, TH, D), bf), sd((4, 2, 2 * FF, D), bf), sd((D,), f32), *[sd((128, D), bf)] * 5),
            in_specs=[hbm] * 5,
            out_specs=[hbm] * 20,
            scratch_shapes=[
                pltpu.VMEM((4, 2, NH, 2, TH, D), bf),
                pltpu.VMEM((2, FF, D), bf),
                pltpu.VMEM((2, 2, NB, D), bf),
                pltpu.VMEM((2, TOK, D), f32),
                pltpu.VMEM((2, FF, D), f32),
                pltpu.VMEM((D,), f32),
                pltpu.VMEM((8, 1, D), f32),
                pltpu.VMEM((8, D), f32),
                pltpu.VMEM((D,), f32),
                dma((6,)),
                dma((9,)),
                dma((2,)),
                dma((4, 3)),
                dma((4, 2, NH)),
                dma((4, 5)),
                dma((4, 4)),
                dma((4,)),
            ],
            compiler_params=pltpu.CompilerParams(collective_id=0, has_side_effects=True, vmem_limit_bytes=VM1),
        )(*(pltpu.with_memory_space_constraint(v, pltpu.HBM) for v in (X, gamma, W1, W2, dY)))
        return pl.pallas_call(
            _finish,
            name="mlp_finish",
            out_shape=(sd((TOK, D), bf), sd((TOK, D), bf), sd((D, FF), f32), sd((FF, D), f32), sd((D,), f32)),
            in_specs=[vm] * 20,
            out_specs=[hbm] * 5,
            scratch_shapes=[
                pltpu.VMEM((D, FF), f32),
                pltpu.VMEM((FF, D), f32),
                dma((3 + 2 * len(STRIPS),)),
            ],
            compiler_params=pltpu.CompilerParams(vmem_limit_bytes=VM2),
        )(pq[10], W2, *pq[:10], *pq[13:], Yp, dXp, pq[12])

    return jax.shard_map(body, mesh=mesh,
                         in_specs=(rows, P(None), P(None, "tp"), P("tp", None), rows),
                         out_specs=(rows, rows, P("data", "tp"), rows, P("data")),
                         check_vma=False)
```
